32 devices in a mesh: dp: 4 (over z), rows: 8 (over y, x, core).
Axes of the slice: x: 2, y: 2, z: 4, core: 2. Of those that a mesh axis runs over, the one named last changes fastest.
Arguments:
- owners: int32 [32768, 1], P(('dp', 'rows')), may hold values from 0 to 31; in each aligned block of 1024 rows (0 to 1023, 1024 to 2047, ...) at most 128 rows name the same one
- offsets: int32 [32768], P(('dp', 'rows')), may hold values from 0 to 8191
- gradients: bfloat16 [32768, 128], P(('dp', 'rows')), may hold values from -6 to 6
- embedding: float32 [262144, 128], P(('dp', 'rows')), may hold values from -6 to 6
- adagrad_state: float32 [262144], P(('dp', 'rows')), may hold values from 0.05 to 2
- next_owners: int32 [32768, 1], P(('dp', 'rows')), may hold values from 0 to 31; in each aligned block of 1024 rows (0 to 1023, 1024 to 2047, ...) at most 128 rows name the same one
- next_offsets: int32 [32768], P(('dp', 'rows')), may hold values from 0 to 8191
Outputs:
- new_embedding: float32 [262144, 128], P(('dp', 'rows'))
- new_state: float32 [262144], P(('dp', 'rows'))
- next_rows: bfloat16 [32768, 128], P(('dp', 'rows'))
The draws below stay inside these ranges and needn't reach their ends.
Inputs may be any that keep to these rules, and one draw needn't show every extreme that they name: `owners`: within the 1024 rows of one device, at most 128 rows name the same block. `next_owners`: within the 1024 rows of one device, at most 128 rows name the same block.
All inputs are finite; a program needn't handle non-finite values.
Results may differ from the reference program's by a relative error of at most 0.0013.
Values may be sent and summed in bfloat16 or wider, within the bound.
A program may use at most 64 MiB of HBM per device.

```python
import math
import jax
import jax.numpy as jnp
import numpy as np
from jax import lax

W = 128
R_DEV = 8192
L_DEV = 1024
V = 262144
LOOKUPS = 32768
CAP = 128
N_DP = 4
N_ROWS = 8


def plant(result, own_key, low, top_value):
    longest = result.shape.index(max(result.shape))
    spots = []
    for shift in (0, 1):
        where = [jax.random.randint(jax.random.fold_in(own_key, axis), (), 0, length) for axis, length in enumerate(result.shape)]
        where[longest] = (where[longest] + shift) % result.shape[longest]
        spots.append(tuple(where))
    return result.at[spots[0]].set(low).at[spots[1]].set(top_value)


def levels(own_key, extent, cuts, least, top_value):
    gain, own = 1.0, jax.random.fold_in(own_key, 6)
    for position, parts in cuts:
        steps = jnp.exp(jax.random.uniform(jax.random.fold_in(own, position), (parts,), jnp.float32, least / len(cuts), top_value / len(cuts)))
        gain = gain * jnp.repeat(steps, extent[position] // parts).reshape([-1 if axis == position else 1 for axis in range(len(extent))])
    return gain


def cumulative_ranks(count, lean):
    loads = [(1 << 20) // math.isqrt(rank ** lean) + 1 for rank in range(1, count + 1)]
    deviation = 1 + sum(loads) // (1 << 30)
    return np.cumsum(np.array([max(1, weight // deviation) for weight in loads]))


def ranked_ids(rng, dims, count, slope):
    listing = cumulative_ranks(count, slope)
    ticket = jax.random.randint(jax.random.fold_in(rng, 1), dims, 0, int(listing[count - 1]))
    rank = jnp.searchsorted(jnp.asarray(listing, jnp.int32), ticket, side="right")
    return jax.random.permutation(jax.random.fold_in(rng, 2), count)[rank].astype(jnp.int32)


def deal_out(stream_key, own, number, rows, count, top, bound, skew):
    sequence = jax.random.permutation(stream_key, count)
    packed, common = portions_of(count, rows * top, bound, skew, True), portions_of(count, rows * top, bound, skew, False)
    places = jnp.arange(count)

    def named(lengths, rotation):
        used = int((lengths > 0).sum())
        fixed = max(1, used // 4)
        shifted = fixed + (places - fixed + rotation * (used - fixed)) % max(1, count - fixed)
        return jnp.zeros((count,), jnp.int32).at[sequence[jnp.where(places < fixed, places, shifted)]].set(jnp.asarray(lengths, jnp.int32))

    lengths = jnp.where(number % 4 == 0, named(packed, number // 4), named(common, number - number // 4 - 1))
    mixed = jax.random.permutation(jax.random.fold_in(own, 3), count)
    giver, receiver = mixed[0:count // 2 * 2:2], mixed[1:count // 2 * 2:2]
    room = jnp.minimum(lengths[giver] - 1, bound - lengths[receiver]) // 2
    room = jnp.where((giver == sequence[0]) | (receiver == sequence[0]) | (lengths[receiver] == 0), 0, jnp.maximum(room, 0))
    shifted = jax.random.randint(jax.random.fold_in(own, 4), (count // 2,), 0, 1 << 20) % (room + 1)
    lengths = lengths.at[giver].add(-shifted).at[receiver].add(shifted)
    items = jnp.searchsorted(jnp.cumsum(lengths), jnp.arange(rows * top), side="right").astype(jnp.int32)
    grid = items.reshape(top, rows).T
    grid = grid[jax.random.permutation(jax.random.fold_in(own, 1), rows)]
    rotation = jax.random.randint(jax.random.fold_in(own, 2), (rows, 1), 0, top)
    return jnp.take_along_axis(grid, (jnp.arange(top)[None, :] + rotation) % top, axis=1)


def portions_of(count, total, bound, lean, full):
    portions = [(1 << 20) // math.isqrt(standing ** lean) + 1 for standing in range(1, count + 1)]
    largest = bound if full else min(bound, max(-(-total // count), total * portions[0] // sum(portions)))
    least = 1 if total - largest >= count - 1 else 0
    counts, spare = [largest] + [least] * (count - 1), total - largest - least * (count - 1)
    while spare > 0:
        movable = [i for i in range(1, count) if counts[i] < largest] or [i for i in range(1, count) if counts[i] < bound]
        pool, budget = sum([portions[i] for i in movable]), spare
        for i in movable:
            extra = min(bound - counts[i], max(1, budget * portions[i] // pool), spare)
            counts[i] = counts[i] + extra
            spare = spare - extra
    return np.array(counts)


def centred(rng, dims, spread, most, cuts=(), dtype=jnp.bfloat16):
    values = jax.random.normal(rng, dims, jnp.float32) * spread
    if len(cuts) > 0:
        values = levels(rng, dims, cuts, -0.22, 0.18) * values
    return jnp.clip(values, min=-most, max=most).astype(dtype)


def setup_inputs(seed: int = 0) -> dict:
    key_list = jax.random.split(jax.random.key(seed), 8)
    owners_keys = jax.random.split(jax.random.fold_in(key_list[0], 1), LOOKUPS // L_DEV)
    owners_turns = jax.random.permutation(jax.random.fold_in(key_list[0], 3), LOOKUPS // L_DEV)
    owners = jax.vmap(lambda own, number: deal_out(jax.random.fold_in(key_list[0], 2), own, number, L_DEV, N_DP * N_ROWS, 1, CAP, 2))(owners_keys, owners_turns).reshape((LOOKUPS, 1))
    offsets = plant(ranked_ids(key_list[1], (LOOKUPS,), R_DEV, 2), jax.random.fold_in(key_list[1], 3), 0, R_DEV - 1).astype(jnp.int32)
    gradients = centred(key_list[2], (LOOKUPS, W), 1.0, 6.0, ((0, 32),))
    embedding = centred(key_list[3], (V, W), 1.0, 6.0, ((0, 32),), jnp.float32)
    adagrad_state = jnp.clip(jnp.exp(math.log(2.0) - 3.6888794 * jax.random.uniform(key_list[4], (V,), jnp.float32) ** levels(key_list[4], (V,), ((0, 32),), -0.2, 0.2)), 0.05, 2.0)
    next_owners_keys = jax.random.split(jax.random.fold_in(key_list[5], 1), LOOKUPS // L_DEV)
    next_owners_turns = jax.random.permutation(jax.random.fold_in(key_list[5], 3), LOOKUPS // L_DEV)
    next_owners = jax.vmap(lambda own, number: deal_out(jax.random.fold_in(key_list[5], 2), own, number, L_DEV, N_DP * N_ROWS, 1, CAP, 2))(next_owners_keys, next_owners_turns).reshape((LOOKUPS, 1))
    next_offsets = plant(ranked_ids(key_list[6], (LOOKUPS,), R_DEV, 2), jax.random.fold_in(key_list[6], 3), 0, R_DEV - 1).astype(jnp.int32)
    return {"owners": owners, "offsets": offsets, "gradients": gradients, "embedding": embedding, "adagrad_state": adagrad_state, "next_owners": next_owners, "next_offsets": next_offsets}


def reference(owners, offsets, gradients, embedding, adagrad_state, next_owners, next_offsets):
    row_ids = (owners[:, 0] * R_DEV + offsets).astype(jnp.int32)
    grad_sum = jnp.zeros((V, W), jnp.float32).at[row_ids].add(gradients.astype(jnp.float32))
    new_state = adagrad_state + lax.optimization_barrier(jnp.mean(grad_sum * grad_sum, axis=1))
    new_embedding = embedding - 0.5 * grad_sum / jnp.sqrt(new_state)[:, None]
    next_ids = (next_owners[:, 0] * R_DEV + next_offsets).astype(jnp.int32)
    next_rows = new_embedding[next_ids].astype(jnp.bfloat16)
    return (new_embedding, new_state, next_rows)
```

```python
import functools

import jax
import jax.numpy as jnp
from jax import lax
from jax.experimental import pallas as pl
from jax.experimental.pallas import tpu as pltpu
from jax.sharding import PartitionSpec as P

LANES = 128
SUB = 16
BASE = 256
MESH = pl.DeviceIdType.MESH


def positions_of(owner_ids, next_ids, devices):
    lookups = owner_ids.shape[0]
    names = jnp.arange(devices, dtype=jnp.int32)[None, :]
    one_hot = jnp.concatenate(
        [owner_ids[:, None] == names, next_ids[:, None] == names], axis=1
    ).astype(jnp.bfloat16)
    index = jnp.arange(lookups, dtype=jnp.int32)
    earlier = (index[:, None] > index[None, :]).astype(jnp.bfloat16)
    ahead = jnp.dot(earlier, one_hot, preferred_element_type=jnp.float32)
    hits = ahead * one_hot.astype(jnp.float32)
    slots = jnp.sum(hits[:, :devices], axis=1), jnp.sum(hits[:, devices:], axis=1)
    return tuple(part.astype(jnp.int32) for part in slots)


def slot_table(owner_ids, slot_ids, values, devices, capacity):
    names = jnp.arange(devices, dtype=jnp.int32)[None, :]
    one_hot = (owner_ids[:, None] == names).astype(jnp.bfloat16)
    in_slot = slot_ids[:, None] == jnp.arange(capacity, dtype=jnp.int32)[None, :]
    columns = jnp.concatenate(
        [jnp.where(in_slot, value.astype(jnp.float32)[:, None], 0.0) for value in values],
        axis=1,
    ).astype(jnp.bfloat16)
    table = lax.dot_general(
        one_hot, columns, (((0,), (0,)), ((), ())), preferred_element_type=jnp.float32
    )
    return table.reshape(devices, len(values), capacity)


def plane_order(dp):
    middle = dp // 2
    return [middle] + [d for d in range(1, dp) if d != middle] + [0]


def peer(dp, rows, dz, dr, sign):
    z, r = lax.axis_index("dp"), lax.axis_index("rows")
    if sign > 0:
        return (lax.rem(z + dz, dp), lax.rem(r + dr, rows))
    return (lax.rem(z + dp - dz, dp), lax.rem(r + rows - dr, rows))


def greet(dp, rows):
    barrier = pltpu.get_barrier_semaphore()

    @pl.loop(1, dp * rows)
    def _(i):
        pl.semaphore_signal(
            barrier,
            inc=1,
            device_id=peer(dp, rows, lax.div(i, rows), lax.rem(i, rows), 1),
            device_id_type=MESH,
        )


def gathered(dp, rows):
    pl.semaphore_wait(pltpu.get_barrier_semaphore(), dp * rows - 1)


def send_kernel(
    dp, rows,
    place_ref, gradients_ref, meta_ref,
    acc_ref, met_ref,
    outgoing, incoming, meta_send, meta_recv, data_send, data_recv,
):
    devices = dp * rows
    slots = outgoing.shape[0]
    capacity = slots // devices
    columns = gradients_ref.shape[1]
    half = acc_ref.shape[0]
    group = 2 if capacity == LANES else 1
    depth = group * capacity

    greet(dp, rows)

    made = 512
    place = place_ref[...]
    lookups = place.shape[1]

    @pl.loop(0, slots // made)
    def _(step):
        start = pl.multiple_of(step * made, made)
        names = lax.broadcasted_iota(jnp.int32, (made, lookups), 0) + start
        chosen = jnp.where(names == place, 1.0, 0.0).astype(jnp.bfloat16)
        outgoing[pl.ds(start, made), :] = jnp.dot(
            chosen, gradients_ref[...], preferred_element_type=jnp.float32
        ).astype(jnp.bfloat16)

    @pl.loop(0, half // LANES)
    def _(step):
        acc_ref[pl.ds(pl.multiple_of(step * LANES, LANES), LANES), :] = jnp.zeros(
            (LANES, acc_ref.shape[1]), jnp.float32
        )

    gathered(dp, rows)

    def copies(dz, dr, sign):
        i = dz * rows + dr
        span = pl.ds(pl.multiple_of(i * capacity, capacity), capacity)
        to = peer(dp, rows, dz, dr, sign)
        meta = pltpu.make_async_remote_copy(
            src_ref=meta_ref.at[i], dst_ref=met_ref.at[i],
            send_sem=meta_send.at[i], recv_sem=meta_recv.at[i],
            device_id=to, device_id_type=MESH,
        )
        data = pltpu.make_async_remote_copy(
            src_ref=outgoing.at[span, :], dst_ref=incoming.at[span, :],
            send_sem=data_send.at[i], recv_sem=data_recv.at[i],
            device_id=to, device_id_type=MESH,
        )
        return meta, data

    for dz in plane_order(dp):

        @pl.loop(0 if dz else 1, rows)
        def _(dr):
            meta, data = copies(dz, dr, 1)
            meta.start()
            data.start()

    met_ref[0] = meta_ref[0]
    incoming[0:capacity, :] = outgoing[0:capacity, :]

    chunk = min(1024, half)
    names = chunk // SUB

    def accumulate(tile):
        met = [met_ref[tile * group + k].astype(jnp.float32) for k in range(group)]
        high = jnp.concatenate([m[0:1, :] for m in met], axis=1)
        both = jnp.concatenate([m[1:2, :] for m in met], axis=1)
        low = jnp.where(both >= SUB, both - SUB, both)
        ones = jnp.where(
            lax.broadcasted_iota(jnp.int32, (SUB, depth), 0).astype(jnp.float32) == low, 1.0, 0.0
        ).astype(jnp.bfloat16)
        parts = []
        for k in range(group):
            upper = jnp.broadcast_to(met[k][1:2, :], (columns, capacity)).T >= SUB
            start = pl.multiple_of((tile * group + k) * capacity, capacity)
            block = incoming[pl.ds(start, capacity), :].astype(jnp.float32)
            parts.append(
                jnp.concatenate(
                    [jnp.where(upper, 0.0, block), jnp.where(upper, block, 0.0)], axis=1
                ).astype(jnp.bfloat16)
            )
        wide = jnp.concatenate(parts, axis=0) if group > 1 else parts[0]
        high = jnp.broadcast_to(high, (SUB, depth))

        @pl.loop(0, half // chunk)
        def _(step):
            shifted = (high - (step * names).astype(jnp.float32)).astype(jnp.bfloat16)
            zero = jnp.zeros((SUB, depth), jnp.bfloat16)
            chosen = jnp.concatenate(
                [jnp.where(shifted == jnp.bfloat16(name), ones, zero) for name in range(names)], axis=0
            )
            span = pl.ds(pl.multiple_of(step * chunk, chunk), chunk)
            acc_ref[span, :] += jnp.dot(chosen, wide, preferred_element_type=jnp.float32)

    per_plane = rows // group
    for dz in plane_order(dp):

        @pl.loop(0, per_plane)
        def _(step):
            for k in range(group):
                dr = step * group + k

                def arrive():
                    meta, data = copies(dz, dr, -1)
                    meta.wait_recv()
                    data.wait_recv()

                if dz == 0:
                    pl.when(dr > 0)(arrive)
                else:
                    arrive()
            accumulate(dz * per_plane + step)

    for dz in plane_order(dp):

        @pl.loop(0 if dz else 1, rows)
        def _(dr):
            meta, data = copies(dz, dr, 1)
            meta.wait_send()
            data.wait_send()


def send_gradients(dp, rows, place, gradients, meta, owned):
    devices, _, capacity = meta.shape
    slots = devices * capacity
    columns = gradients.shape[1]
    vmem = pl.BlockSpec(memory_space=pltpu.VMEM)
    return pl.pallas_call(
        functools.partial(send_kernel, dp, rows),
        name="send_gradients",
        out_shape=(
            jax.ShapeDtypeStruct((owned // 2, 2 * columns), jnp.float32),
            jax.ShapeDtypeStruct(meta.shape, meta.dtype),
        ),
        in_specs=[vmem] * 3,
        out_specs=(vmem, vmem),
        scratch_shapes=[
            pltpu.VMEM((slots, columns), jnp.bfloat16),
            pltpu.VMEM((slots, columns), jnp.bfloat16),
        ]
        + [pltpu.SemaphoreType.DMA((devices,))] * 4,
        compiler_params=pltpu.CompilerParams(
            collective_id=0, has_side_effects=True, vmem_limit_bytes=32 * 1024 * 1024
        ),
    )(place.reshape(1, -1), gradients, meta)


def update_kernel(
    acc_ref, embedding_ref, state_ref, new_embedding_ref, new_state_ref, table, in_sems, out_sems
):
    owned = table.shape[0]
    half = acc_ref.shape[0]
    chunks = in_sems.shape[0]
    chunk = owned // chunks

    def load(piece):
        span = pl.ds(piece * chunk, chunk)
        return pltpu.make_async_copy(embedding_ref.at[span, :], table.at[span, :], in_sems.at[piece])

    def store(piece):
        span = pl.ds(piece * chunk, chunk)
        return pltpu.make_async_copy(
            table.at[span, :], new_embedding_ref.at[span, :], out_sems.at[piece]
        )

    for piece in range(chunks):
        load(piece).start()
    for piece in range(chunks):
        load(piece).wait()
        side = piece * chunk // half

        @pl.loop(0, chunk // LANES, unroll=4)
        def _(step):
            tile = piece * (chunk // LANES) + step
            span = pl.ds(pl.multiple_of(tile * LANES, LANES), LANES)
            low = pl.ds(pl.multiple_of(tile * LANES - side * half, LANES), LANES)
            grad_sum = acc_ref[low, side * LANES : (side + 1) * LANES]
            mean = jnp.sum(grad_sum * grad_sum, axis=1, keepdims=True) * (1.0 / LANES)
            old = jnp.broadcast_to(state_ref[pl.ds(tile, 1), :], (LANES, LANES)).T
            state = old + mean
            new_state_ref[pl.ds(tile, 1), :] = state.T[0:1, :]
            table[span, :] = table[span, :] - 0.5 * grad_sum * lax.rsqrt(state)

        store(piece).start()
    for piece in range(chunks):
        store(piece).wait()


def update(acc, embedding, state):
    owned, columns = embedding.shape
    chunks = 8
    vmem = pl.BlockSpec(memory_space=pltpu.VMEM)
    hbm = pl.BlockSpec(memory_space=pltpu.HBM)
    new_embedding, new_state, table = pl.pallas_call(
        update_kernel,
        name="update",
        out_shape=(
            jax.ShapeDtypeStruct((owned, columns), jnp.float32),
            jax.ShapeDtypeStruct((owned // LANES, LANES), jnp.float32),
            jax.ShapeDtypeStruct((owned, columns), jnp.float32),
        ),
        in_specs=[vmem, hbm, vmem],
        out_specs=(hbm, vmem, vmem),
        scratch_shapes=[
            pltpu.SemaphoreType.DMA((chunks,)),
            pltpu.SemaphoreType.DMA((chunks,)),
        ],
        compiler_params=pltpu.CompilerParams(vmem_limit_bytes=32 * 1024 * 1024),
    )(acc, embedding, state.reshape(owned // LANES, LANES))
    return new_embedding, new_state.reshape(owned), table


def fetch_kernel(
    dp, rows,
    wanted_hbm, place_ref, table_ref, next_ref,
    wanted_ref, picked, outgoing, incoming, total, wanted_sem, data_send, data_recv,
):
    devices = dp * rows
    slots = outgoing.shape[0]
    capacity = slots // devices
    group = 2 if capacity == LANES else 1
    depth = group * capacity

    greet(dp, rows)
    load = pltpu.make_async_copy(wanted_hbm, wanted_ref, wanted_sem)
    load.start()
    total[...] = jnp.zeros(total.shape, jnp.float32)
    load.wait()

    def copy(dz, dr, sign):
        i = dz * rows + dr
        span = pl.ds(pl.multiple_of(i * capacity, capacity), capacity)
        return pltpu.make_async_remote_copy(
            src_ref=outgoing.at[span, :], dst_ref=incoming.at[span, :],
            send_sem=data_send.at[i], recv_sem=data_recv.at[i],
            device_id=peer(dp, rows, dz, dr, sign), device_id_type=MESH,
        )

    def gather(i):
        start = pl.multiple_of(i * capacity, capacity)
        for k in range(capacity):
            picked[pl.ds(k, 1), :] = table_ref[pl.ds(wanted_ref[start + k], 1), :]
        outgoing[pl.ds(start, capacity), :] = picked[...].astype(jnp.bfloat16)

    for position, dz in enumerate(plane_order(dp)):

        @pl.loop(0, rows)
        def _(dr):
            gather(dz * rows + dr)

        if position == 0:
            gathered(dp, rows)

        @pl.loop(0 if dz else 1, rows)
        def _(dr):
            copy(dz, dr, -1).start()

    incoming[0:capacity, :] = outgoing[0:capacity, :]

    lookups = total.shape[0]
    place = jnp.broadcast_to(place_ref[...], (lookups, depth)) - lax.broadcasted_iota(
        jnp.int32, (lookups, depth), 1
    )

    per_plane = rows // group
    for dz in plane_order(dp):

        @pl.loop(0, per_plane)
        def _(step):
            for k in range(group):
                dr = step * group + k

                def arrive():
                    copy(dz, dr, 1).wait_recv()

                if dz == 0:
                    pl.when(dr > 0)(arrive)
                else:
                    arrive()
            start = pl.multiple_of((dz * per_plane + step) * depth, depth)
            chosen = jnp.where(place == start, 1.0, 0.0).astype(jnp.bfloat16)
            total[...] += jnp.dot(
                chosen, incoming[pl.ds(start, depth), :], preferred_element_type=jnp.float32
            )

    next_ref[...] = total[...].astype(jnp.bfloat16)

    for dz in plane_order(dp):

        @pl.loop(0 if dz else 1, rows)
        def _(dr):
            copy(dz, dr, -1).wait_send()


def fetch(dp, rows, wanted, place, table):
    slots = wanted.shape[0]
    devices = dp * rows
    lookups = place.shape[0]
    columns = table.shape[1]
    vmem = pl.BlockSpec(memory_space=pltpu.VMEM)
    hbm = pl.BlockSpec(memory_space=pltpu.HBM)
    return pl.pallas_call(
        functools.partial(fetch_kernel, dp, rows),
        name="fetch",
        out_shape=jax.ShapeDtypeStruct((lookups, columns), jnp.bfloat16),
        in_specs=[hbm, vmem, vmem],
        out_specs=vmem,
        scratch_shapes=[
            pltpu.SMEM((slots,), jnp.int32),
            pltpu.VMEM((slots // devices, columns), jnp.float32),
            pltpu.VMEM((slots, columns), jnp.bfloat16),
            pltpu.VMEM((slots, columns), jnp.bfloat16),
            pltpu.VMEM((lookups, columns), jnp.float32),
            pltpu.SemaphoreType.DMA,
            pltpu.SemaphoreType.DMA((devices,)),
            pltpu.SemaphoreType.DMA((devices,)),
        ],
        compiler_params=pltpu.CompilerParams(
            collective_id=1, has_side_effects=True, vmem_limit_bytes=32 * 1024 * 1024
        ),
    )(wanted, place.reshape(-1, 1), table)


def on_device(owners, offsets, gradients, embedding, adagrad_state, next_owners, next_offsets):
    dp, rows = lax.axis_size("dp"), lax.axis_size("rows")
    devices = dp * rows
    lookups = gradients.shape[0]
    owned = embedding.shape[0]
    capacity = max(2, 4 * lookups // devices)
    z, r = lax.axis_index("dp"), lax.axis_index("rows")

    def relative(names):
        dz = (names // rows - z + dp) % dp
        dr = (names % rows - r + rows) % rows
        return dz * rows + dr

    owner_ids, next_ids = relative(owners[:, 0]), relative(next_owners[:, 0])
    slot_ids, next_slots = positions_of(owner_ids, next_ids, devices)
    places = owner_ids * capacity + slot_ids
    next_places = next_ids * capacity + next_slots
    half = owned // 2
    high = (offsets % half) // SUB
    both = (offsets // half) * SUB + offsets % SUB
    table = slot_table(owner_ids, slot_ids, (high, both), devices, capacity)
    next_table = slot_table(
        next_ids, next_slots, (next_offsets // BASE, next_offsets % BASE), devices, capacity
    )
    meta = jnp.concatenate([table, next_table], axis=1).astype(jnp.bfloat16)
    acc, met = send_gradients(dp, rows, places, gradients, meta, owned)
    wanted = (met[:, 2].astype(jnp.int32) * BASE + met[:, 3].astype(jnp.int32)).reshape(-1)
    new_embedding, new_state, new_table = update(acc, embedding, adagrad_state)
    next_rows = fetch(dp, rows, wanted, next_places, new_table)
    return (new_embedding, new_state, next_rows)


def solution(mesh):
    in_specs = (
        P(("dp", "rows"), None),
        P(("dp", "rows")),
        P(("dp", "rows"), None),
        P(("dp", "rows"), None),
        P(("dp", "rows")),
        P(("dp", "rows"), None),
        P(("dp", "rows")),
    )
    out_specs = (P(("dp", "rows"), None), P(("dp", "rows")), P(("dp", "rows"), None))
    return jax.shard_map(
        on_device, mesh=mesh, in_specs=in_specs, out_specs=out_specs, check_vma=False
    )
```

```python
import functools

import jax
import jax.numpy as jnp
from jax import lax
from jax.experimental import pallas as pl
from jax.experimental.pallas import tpu as pltpu
from jax.sharding import PartitionSpec as P

LANES = 128
SUB = 16
BASE = 256
MESH = pl.DeviceIdType.MESH


def flip(value, step, size):
    bit, result = 1, value
    while bit < size:
        own = lax.rem(lax.div(value, bit), 2)
        if isinstance(step, int):
            if step // bit % 2:
                result = result + bit * (1 - 2 * own)
        else:
            other = lax.rem(lax.div(step, bit), 2)
            result = result + bit * other * (1 - 2 * own)
        bit *= 2
    return result


def plane_order(dp):
    return [0, 1] + list(range(dp - 1, 1, -1))


def peer(dp, rows, dz, dr):
    z, r = lax.axis_index("dp"), lax.axis_index("rows")
    return (flip(z, dz, dp), flip(r, dr, rows))


def greet(dp, rows):
    barrier = pltpu.get_barrier_semaphore()
    for i in range(1, dp * rows):
        pl.semaphore_signal(
            barrier, inc=1, device_id=peer(dp, rows, i // rows, i % rows), device_id_type=MESH
        )


def gathered(dp, rows):
    pl.semaphore_wait(pltpu.get_barrier_semaphore(), dp * rows - 1)


def selectors(names, count):
    shape = (SUB, names.shape[1])
    low = lax.broadcasted_iota(jnp.int32, shape, 0) == names % SUB
    ones = jnp.where(low, 1.0, 0.0).astype(jnp.bfloat16)
    high = jnp.broadcast_to((names // SUB).astype(jnp.float32), shape)

    def pick(start):
        shifted = (high - start).astype(jnp.bfloat16)
        zero = jnp.zeros(shape, jnp.bfloat16)
        return jnp.concatenate(
            [jnp.where(shifted == jnp.bfloat16(k), ones, zero) for k in range(count // SUB)], axis=0
        )

    return pick


def route(names, values, me, devices, capacity):
    blocks = names.shape[0]
    columns = names.shape[1]
    relative = jnp.bitwise_xor(names, me)
    index = lax.broadcasted_iota(jnp.int32, (devices, columns), 0)
    hits = [jnp.where(index == relative[b : b + 1, :], 1.0, 0.0) for b in range(blocks)]
    before = jnp.where(
        lax.broadcasted_iota(jnp.int32, (columns, columns), 0)
        < lax.broadcasted_iota(jnp.int32, (columns, columns), 1),
        1.0,
        0.0,
    ).astype(jnp.bfloat16)
    one_hot = [hit.astype(jnp.bfloat16) for hit in hits]
    ahead = jnp.dot(
        jnp.concatenate(one_hot, axis=0), before, preferred_element_type=jnp.float32
    )
    seen = jnp.zeros((devices, 1), jnp.float32)
    slots = []
    for b in range(blocks):
        within = ahead[b * devices : (b + 1) * devices, :] + seen
        slots.append(jnp.sum(hits[b] * within, axis=0, keepdims=True))
        seen = seen + jnp.sum(hits[b], axis=1, keepdims=True)
    slots = jnp.concatenate(slots, axis=0).astype(jnp.int32)
    high = (values // BASE).astype(jnp.float32)
    low = (values % BASE).astype(jnp.float32)
    place = lax.broadcasted_iota(jnp.int32, (capacity, columns), 0)
    marked = []
    for b in range(blocks):
        taken = place == slots[b : b + 1, :]
        marked.append(
            jnp.concatenate(
                [jnp.where(taken, high[b : b + 1, :], 0.0), jnp.where(taken, low[b : b + 1, :], 0.0)],
                axis=0,
            ).astype(jnp.bfloat16)
        )
    table = lax.dot_general(
        jnp.concatenate(one_hot, axis=1),
        jnp.concatenate(marked, axis=1),
        (((1,), (1,)), ((), ())),
        preferred_element_type=jnp.float32,
    )
    table = (table[:, :capacity] * BASE + table[:, capacity:]).astype(jnp.int32)
    return relative * capacity + slots, table


def send_kernel(
    dp, rows,
    owners_ref, offsets_ref, next_owners_ref, next_offsets_ref, gradients_ref,
    acc_ref, met_ref, next_place_ref,
    flat, meta_ref, outgoing, incoming, meta_send, meta_recv, data_send, data_recv,
):
    devices = dp * rows
    slots = outgoing.shape[0]
    capacity = slots // devices
    columns = gradients_ref.shape[1]
    half = acc_ref.shape[0]
    group = 2 if capacity == LANES else 1
    depth = group * capacity

    greet(dp, rows)

    me = lax.axis_index("dp") * rows + lax.axis_index("rows")
    place, table = route(owners_ref[...], offsets_ref[...], me, devices, capacity)
    next_place, next_table = route(
        next_owners_ref[...], next_offsets_ref[...], me, devices, capacity
    )
    next_place_ref[...] = next_place
    flat[...] = jnp.concatenate([table, next_table], axis=1)
    for i in range(devices):
        meta_ref[i] = flat[i : i + 1, :]

    made = min(512, slots)
    pick = selectors(
        jnp.concatenate([place[b : b + 1, :] for b in range(place.shape[0])], axis=1), made
    )

    @pl.loop(0, slots // made)
    def _(step):
        start = pl.multiple_of(step * made, made)
        outgoing[pl.ds(start, made), :] = jnp.dot(
            pick((step * (made // SUB)).astype(jnp.float32)),
            gradients_ref[...],
            preferred_element_type=jnp.float32,
        ).astype(jnp.bfloat16)

    @pl.loop(0, half // LANES)
    def _(step):
        acc_ref[pl.ds(pl.multiple_of(step * LANES, LANES), LANES), :] = jnp.zeros(
            (LANES, acc_ref.shape[1]), jnp.float32
        )

    gathered(dp, rows)

    def copies(dz, dr):
        i = dz * rows + dr
        span = pl.ds(pl.multiple_of(i * capacity, capacity), capacity)
        to = peer(dp, rows, dz, dr)
        meta = pltpu.make_async_remote_copy(
            src_ref=meta_ref.at[i], dst_ref=met_ref.at[i],
            send_sem=meta_send.at[i], recv_sem=meta_recv.at[i],
            device_id=to, device_id_type=MESH,
        )
        data = pltpu.make_async_remote_copy(
            src_ref=outgoing.at[span, :], dst_ref=incoming.at[span, :],
            send_sem=data_send.at[i], recv_sem=data_recv.at[i],
            device_id=to, device_id_type=MESH,
        )
        return meta, data

    for dz in plane_order(dp):
        for dr in range(0 if dz else 1, rows):
            meta, data = copies(dz, dr)
            meta.start()
            data.start()

    met_ref[0] = meta_ref[0]
    incoming[0:capacity, :] = outgoing[0:capacity, :]

    chunk = min(1024, half)

    def accumulate(tile):
        met = [met_ref[tile * group + k][:, :capacity] for k in range(group)]
        parts = []
        for k in range(group):
            side = jnp.broadcast_to((met[k] // half).astype(jnp.float32), (columns, capacity)).T
            start = pl.multiple_of((tile * group + k) * capacity, capacity)
            block = incoming[pl.ds(start, capacity), :].astype(jnp.float32)
            parts.append(
                jnp.concatenate(
                    [jnp.where(side > 0.5, 0.0, block), jnp.where(side > 0.5, block, 0.0)], axis=1
                ).astype(jnp.bfloat16)
            )
        wide = jnp.concatenate(parts, axis=0) if group > 1 else parts[0]
        names = (jnp.concatenate(met, axis=1) if group > 1 else met[0]) % half
        pick_rows = selectors(names, chunk)

        @pl.loop(0, half // chunk)
        def _(step):
            span = pl.ds(pl.multiple_of(step * chunk, chunk), chunk)
            acc_ref[span, :] += jnp.dot(
                pick_rows((step * (chunk // SUB)).astype(jnp.float32)),
                wide,
                preferred_element_type=jnp.float32,
            )

    per_plane = rows // group
    for dz in plane_order(dp):

        @pl.loop(0, per_plane)
        def _(step):
            for k in range(group):
                dr = step * group + k

                def arrive():
                    meta, data = copies(dz, dr)
                    meta.wait_recv()
                    data.wait_recv()

                if dz == 0:
                    pl.when(dr > 0)(arrive)
                else:
                    arrive()
            accumulate(dz * per_plane + step)

    for dz in plane_order(dp):

        @pl.loop(0 if dz else 1, rows)
        def _(dr):
            meta, data = copies(dz, dr)
            meta.wait_send()
            data.wait_send()


def send_gradients(dp, rows, owners, offsets, next_owners, next_offsets, gradients, owned):
    devices = dp * rows
    lookups, columns = gradients.shape
    capacity = max(2, 4 * lookups // devices)
    slots = devices * capacity
    vmem = pl.BlockSpec(memory_space=pltpu.VMEM)
    tiles = (lookups // LANES, LANES)
    return pl.pallas_call(
        functools.partial(send_kernel, dp, rows),
        name="send_gradients",
        out_shape=(
            jax.ShapeDtypeStruct((owned // 2, 2 * columns), jnp.float32),
            jax.ShapeDtypeStruct((devices, 1, 2 * capacity), jnp.int32),
            jax.ShapeDtypeStruct(tiles, jnp.int32),
        ),
        in_specs=[vmem] * 5,
        out_specs=(vmem,) * 3,
        scratch_shapes=[
            pltpu.VMEM((devices, 2 * capacity), jnp.int32),
            pltpu.VMEM((devices, 1, 2 * capacity), jnp.int32),
            pltpu.VMEM((slots, columns), jnp.bfloat16),
            pltpu.VMEM((slots, columns), jnp.bfloat16),
        ]
        + [pltpu.SemaphoreType.DMA((devices,))] * 4,
        compiler_params=pltpu.CompilerParams(
            collective_id=0, has_side_effects=True, vmem_limit_bytes=40 * 1024 * 1024
        ),
        cost_estimate=pl.CostEstimate(
            flops=400 * slots * owned * columns, bytes_accessed=owned * columns * 4, transcendentals=0
        ),
    )(
        owners.reshape(tiles), offsets.reshape(tiles),
        next_owners.reshape(tiles), next_offsets.reshape(tiles),
        gradients,
    )


def update_kernel(
    acc_ref, embedding_ref, state_ref, new_embedding_ref, new_state_ref, table, out_sems
):
    owned = table.shape[0]
    half = acc_ref.shape[0]
    chunks = out_sems.shape[0]
    chunk = owned // chunks

    def store(piece):
        span = pl.ds(piece * chunk, chunk)
        return pltpu.make_async_copy(
            table.at[span, :], new_embedding_ref.at[span, :], out_sems.at[piece]
        )

    for piece in range(chunks):
        side = piece * chunk // half

        @pl.loop(0, chunk // LANES, unroll=4)
        def _(step):
            tile = piece * (chunk // LANES) + step
            span = pl.ds(pl.multiple_of(tile * LANES, LANES), LANES)
            low = pl.ds(pl.multiple_of(tile * LANES - side * half, LANES), LANES)
            grad_sum = acc_ref[low, side * LANES : (side + 1) * LANES]
            mean = jnp.sum(grad_sum * grad_sum, axis=1, keepdims=True) * (1.0 / LANES)
            old = jnp.broadcast_to(state_ref[pl.ds(tile, 1), :], (LANES, LANES)).T
            state = old + mean
            new_state_ref[pl.ds(tile, 1), :] = state.T[0:1, :]
            table[span, :] = embedding_ref[span, :] - 0.5 * grad_sum * lax.rsqrt(state)

        store(piece).start()
    for piece in range(chunks):
        store(piece).wait()


def update(acc, embedding, state):
    owned, columns = embedding.shape
    chunks = 8
    vmem = pl.BlockSpec(memory_space=pltpu.VMEM)
    hbm = pl.BlockSpec(memory_space=pltpu.HBM)
    new_embedding, new_state, table = pl.pallas_call(
        update_kernel,
        name="update",
        out_shape=(
            jax.ShapeDtypeStruct((owned, columns), jnp.float32),
            jax.ShapeDtypeStruct((owned // LANES, LANES), jnp.float32),
            jax.ShapeDtypeStruct((owned, columns), jnp.float32),
        ),
        in_specs=[vmem] * 3,
        out_specs=(hbm, vmem, vmem),
        scratch_shapes=[pltpu.SemaphoreType.DMA((chunks,))],
        compiler_params=pltpu.CompilerParams(vmem_limit_bytes=40 * 1024 * 1024),
    )(acc, embedding, state.reshape(owned // LANES, LANES))
    return new_embedding, new_state.reshape(owned), table


def fetch_kernel(
    dp, rows,
    wanted_hbm, place_ref, table_ref, next_ref,
    wanted_ref, picked, outgoing, incoming, place, total, wanted_sem, data_send, data_recv,
):
    devices = dp * rows
    slots = outgoing.shape[0]
    capacity = slots // devices
    group = 2 if capacity == LANES else 1
    depth = group * capacity

    greet(dp, rows)
    load = pltpu.make_async_copy(wanted_hbm, wanted_ref, wanted_sem)
    load.start()
    total[...] = jnp.zeros(total.shape, jnp.float32)
    for b in range(place_ref.shape[0]):
        row = place_ref[b : b + 1, :].astype(jnp.float32)
        place[b * LANES : (b + 1) * LANES, :] = jnp.broadcast_to(row, (LANES, LANES)).T.astype(
            jnp.int32
        )
    load.wait()

    def copy(dz, dr):
        i = dz * rows + dr
        span = pl.ds(pl.multiple_of(i * capacity, capacity), capacity)
        return pltpu.make_async_remote_copy(
            src_ref=outgoing.at[span, :], dst_ref=incoming.at[span, :],
            send_sem=data_send.at[i], recv_sem=data_recv.at[i],
            device_id=peer(dp, rows, dz, dr), device_id_type=MESH,
        )

    def gather(i):
        start = pl.multiple_of(i * capacity, capacity)
        for k in range(capacity):
            picked[pl.ds(k, 1), :] = table_ref[pl.ds(wanted_ref[start + k], 1), :]
        outgoing[pl.ds(start, capacity), :] = picked[...].astype(jnp.bfloat16)

    for position, dz in enumerate(plane_order(dp)):

        @pl.loop(0, rows)
        def _(dr):
            gather(dz * rows + dr)

        if position == 0:
            gathered(dp, rows)

        for dr in range(0 if dz else 1, rows):
            copy(dz, dr).start()

    incoming[0:capacity, :] = outgoing[0:capacity, :]

    lookups = total.shape[0]

    per_plane = rows // group
    for dz in plane_order(dp):

        @pl.loop(0, per_plane)
        def _(step):
            for k in range(group):
                dr = step * group + k

                def arrive():
                    copy(dz, dr).wait_recv()

                if dz == 0:
                    pl.when(dr > 0)(arrive)
                else:
                    arrive()
            start = pl.multiple_of((dz * per_plane + step) * depth, depth)
            lane = lax.broadcasted_iota(jnp.int32, (lookups, capacity), 1)
            chosen = jnp.concatenate(
                [
                    jnp.where(place[:, :capacity] == lane + (start + k * capacity), 1.0, 0.0)
                    for k in range(group)
                ],
                axis=1,
            ).astype(jnp.bfloat16)
            total[...] += jnp.dot(
                chosen, incoming[pl.ds(start, depth), :], preferred_element_type=jnp.float32
            )

    next_ref[...] = total[...].astype(jnp.bfloat16)

    for dz in plane_order(dp):

        @pl.loop(0 if dz else 1, rows)
        def _(dr):
            copy(dz, dr).wait_send()


def fetch(dp, rows, wanted, place, table):
    slots = wanted.shape[0]
    devices = dp * rows
    lookups = place.shape[0] * place.shape[1]
    columns = table.shape[1]
    vmem = pl.BlockSpec(memory_space=pltpu.VMEM)
    hbm = pl.BlockSpec(memory_space=pltpu.HBM)
    return pl.pallas_call(
        functools.partial(fetch_kernel, dp, rows),
        name="fetch",
        out_shape=jax.ShapeDtypeStruct((lookups, columns), jnp.bfloat16),
        in_specs=[hbm, vmem, vmem],
        out_specs=vmem,
        scratch_shapes=[
            pltpu.SMEM((slots,), jnp.int32),
            pltpu.VMEM((slots // devices, columns), jnp.float32),
            pltpu.VMEM((slots, columns), jnp.bfloat16),
            pltpu.VMEM((slots, columns), jnp.bfloat16),
            pltpu.VMEM((lookups, LANES), jnp.int32),
            pltpu.VMEM((lookups, columns), jnp.float32),
            pltpu.SemaphoreType.DMA,
            pltpu.SemaphoreType.DMA((devices,)),
            pltpu.SemaphoreType.DMA((devices,)),
        ],
        compiler_params=pltpu.CompilerParams(
            collective_id=1, has_side_effects=True, vmem_limit_bytes=32 * 1024 * 1024
        ),
    )(wanted, place, table)


def on_device(owners, offsets, gradients, embedding, adagrad_state, next_owners, next_offsets):
    dp, rows = lax.axis_size("dp"), lax.axis_size("rows")
    acc, met, next_place = send_gradients(
        dp, rows, owners, offsets, next_owners, next_offsets, gradients, embedding.shape[0]
    )
    wanted = met[:, 0, met.shape[2] // 2 :].reshape(-1)
    new_embedding, new_state, new_table = update(acc, embedding, adagrad_state)
    next_rows = fetch(dp, rows, wanted, next_place, new_table)
    return (new_embedding, new_state, next_rows)


def solution(mesh):
    in_specs = (
        P(("dp", "rows"), None),
        P(("dp", "rows")),
        P(("dp", "rows"), None),
        P(("dp", "rows"), None),
        P(("dp", "rows")),
        P(("dp", "rows"), None),
        P(("dp", "rows")),
    )
    out_specs = (P(("dp", "rows"), None), P(("dp", "rows")), P(("dp", "rows"), None))
    return jax.shard_map(
        on_device, mesh=mesh, in_specs=in_specs, out_specs=out_specs, check_vma=False
    )
```

```python
import functools

import jax
import jax.numpy as jnp
from jax import lax
from jax.experimental import pallas as pl
from jax.experimental.pallas import tpu as pltpu
from jax.sharding import PartitionSpec as P

LANES = 128
SUB = 16
BASE = 256
MESH = pl.DeviceIdType.MESH


def flip(value, step, size):
    bit, result = 1, value
    while bit < size:
        own = lax.rem(lax.div(value, bit), 2)
        if isinstance(step, int):
            if step // bit % 2:
                result = result + bit * (1 - 2 * own)
        else:
            other = lax.rem(lax.div(step, bit), 2)
            result = result + bit * other * (1 - 2 * own)
        bit *= 2
    return result


def plane_order(dp):
    return [dp - 1] + list(range(dp - 1))


def peer(dp, rows, dz, dr):
    z, r = lax.axis_index("dp"), lax.axis_index("rows")
    return (flip(z, dz, dp), flip(r, dr, rows))


def greet(dp, rows):
    barrier = pltpu.get_barrier_semaphore()
    for i in range(1, dp * rows):
        pl.semaphore_signal(
            barrier, inc=1, device_id=peer(dp, rows, i // rows, i % rows), device_id_type=MESH
        )


def gathered(dp, rows):
    pl.semaphore_wait(pltpu.get_barrier_semaphore(), dp * rows - 1)


def selectors(names, count):
    shape = (SUB, names.shape[1])
    low = lax.broadcasted_iota(jnp.int32, shape, 0) == names % SUB
    ones = jnp.where(low, 1.0, 0.0).astype(jnp.bfloat16)
    high = jnp.broadcast_to((names // SUB).astype(jnp.float32), shape)

    def pick(start):
        shifted = (high - start).astype(jnp.bfloat16)
        zero = jnp.zeros(shape, jnp.bfloat16)
        return jnp.concatenate(
            [jnp.where(shifted == jnp.bfloat16(k), ones, zero) for k in range(count // SUB)], axis=0
        )

    return pick


def route(names, values, me, devices, capacity):
    blocks = names.shape[0]
    columns = names.shape[1]
    relative = jnp.bitwise_xor(names, me)
    index = lax.broadcasted_iota(jnp.int32, (devices, columns), 0)
    hits = [jnp.where(index == relative[b : b + 1, :], 1.0, 0.0) for b in range(blocks)]
    before = jnp.where(
        lax.broadcasted_iota(jnp.int32, (columns, columns), 0)
        < lax.broadcasted_iota(jnp.int32, (columns, columns), 1),
        1.0,
        0.0,
    ).astype(jnp.bfloat16)
    one_hot = [hit.astype(jnp.bfloat16) for hit in hits]
    ahead = jnp.dot(
        jnp.concatenate(one_hot, axis=0), before, preferred_element_type=jnp.float32
    )
    seen = jnp.zeros((devices, 1), jnp.float32)
    slots = []
    for b in range(blocks):
        within = ahead[b * devices : (b + 1) * devices, :] + seen
        slots.append(jnp.sum(hits[b] * within, axis=0, keepdims=True))
        seen = seen + jnp.sum(hits[b], axis=1, keepdims=True)
    slots = jnp.concatenate(slots, axis=0).astype(jnp.int32)
    high = (values // BASE).astype(jnp.float32)
    low = (values % BASE).astype(jnp.float32)
    place = lax.broadcasted_iota(jnp.int32, (capacity, columns), 0)
    marked = []
    for b in range(blocks):
        taken = place == slots[b : b + 1, :]
        marked.append(
            jnp.concatenate(
                [jnp.where(taken, high[b : b + 1, :], 0.0), jnp.where(taken, low[b : b + 1, :], 0.0)],
                axis=0,
            ).astype(jnp.bfloat16)
        )
    table = lax.dot_general(
        jnp.concatenate(one_hot, axis=1),
        jnp.concatenate(marked, axis=1),
        (((1,), (1,)), ((), ())),
        preferred_element_type=jnp.float32,
    )
    table = (table[:, :capacity] * BASE + table[:, capacity:]).astype(jnp.int32)
    return relative * capacity + slots, table


def send_kernel(
    dp, rows,
    index_ref, gradients_ref,
    acc_ref, met_ref, next_place_ref,
    flat, meta_ref, outgoing, incoming, meta_send, meta_recv, data_send, data_recv,
):
    devices = dp * rows
    slots = outgoing.shape[0]
    capacity = slots // devices
    columns = gradients_ref.shape[1]
    half = acc_ref.shape[0]
    group = 2 if capacity == LANES else 1
    depth = group * capacity

    greet(dp, rows)

    me = lax.axis_index("dp") * rows + lax.axis_index("rows")
    place, table = route(index_ref[0], index_ref[1], me, devices, capacity)
    next_place, next_table = route(index_ref[2], index_ref[3], me, devices, capacity)
    next_place_ref[...] = next_place
    flat[...] = jnp.concatenate([table, next_table], axis=1)
    for i in range(devices):
        meta_ref[i] = flat[i : i + 1, :]

    made = min(512, rows * capacity)
    pick = selectors(
        jnp.concatenate([place[b : b + 1, :] for b in range(place.shape[0])], axis=1), made
    )

    def copies(dz, dr):
        i = dz * rows + dr
        span = pl.ds(pl.multiple_of(i * capacity, capacity), capacity)
        to = peer(dp, rows, dz, dr)
        meta = pltpu.make_async_remote_copy(
            src_ref=meta_ref.at[i], dst_ref=met_ref.at[i],
            send_sem=meta_send.at[i], recv_sem=meta_recv.at[i],
            device_id=to, device_id_type=MESH,
        )
        data = pltpu.make_async_remote_copy(
            src_ref=outgoing.at[span, :], dst_ref=incoming.at[span, :],
            send_sem=data_send.at[i], recv_sem=data_recv.at[i],
            device_id=to, device_id_type=MESH,
        )
        return meta, data

    plane = rows * capacity
    for position, dz in enumerate(plane_order(dp)):

        @pl.loop(dz * plane // made, (dz + 1) * plane // made)
        def _(step):
            start = pl.multiple_of(step * made, made)
            outgoing[pl.ds(start, made), :] = jnp.dot(
                pick((step * (made // SUB)).astype(jnp.float32)),
                gradients_ref[...],
                preferred_element_type=jnp.float32,
            ).astype(jnp.bfloat16)

        if position == 0:
            gathered(dp, rows)

        for dr in range(0 if dz else 1, rows):
            meta, data = copies(dz, dr)
            meta.start()
            data.start()

    @pl.loop(0, half // LANES)
    def _(step):
        acc_ref[pl.ds(pl.multiple_of(step * LANES, LANES), LANES), :] = jnp.zeros(
            (LANES, acc_ref.shape[1]), jnp.float32
        )

    met_ref[0] = meta_ref[0]
    incoming[0:capacity, :] = outgoing[0:capacity, :]

    chunk = min(1024, half)

    def accumulate(tile):
        met = [met_ref[tile * group + k][:, :capacity] for k in range(group)]
        parts = []
        for k in range(group):
            side = jnp.broadcast_to((met[k] // half).astype(jnp.float32), (columns, capacity)).T
            start = pl.multiple_of((tile * group + k) * capacity, capacity)
            block = incoming[pl.ds(start, capacity), :].astype(jnp.float32)
            parts.append(
                jnp.concatenate(
                    [jnp.where(side > 0.5, 0.0, block), jnp.where(side > 0.5, block, 0.0)], axis=1
                ).astype(jnp.bfloat16)
            )
        wide = jnp.concatenate(parts, axis=0) if group > 1 else parts[0]
        names = (jnp.concatenate(met, axis=1) if group > 1 else met[0]) % half
        pick_rows = selectors(names, chunk)

        @pl.loop(0, half // chunk)
        def _(step):
            span = pl.ds(pl.multiple_of(step * chunk, chunk), chunk)
            acc_ref[span, :] += jnp.dot(
                pick_rows((step * (chunk // SUB)).astype(jnp.float32)),
                wide,
                preferred_element_type=jnp.float32,
            )

    per_plane = rows // group
    for dz in plane_order(dp):

        @pl.loop(0, per_plane)
        def _(step):
            for k in range(group):
                dr = step * group + k

                def arrive():
                    meta, data = copies(dz, dr)
                    meta.wait_recv()
                    data.wait_recv()

                if dz == 0:
                    pl.when(dr > 0)(arrive)
                else:
                    arrive()
            accumulate(dz * per_plane + step)

    for dz in plane_order(dp):

        @pl.loop(0 if dz else 1, rows)
        def _(dr):
            meta, data = copies(dz, dr)
            meta.wait_send()
            data.wait_send()


def send_gradients(dp, rows, owners, offsets, next_owners, next_offsets, gradients, owned):
    devices = dp * rows
    lookups, columns = gradients.shape
    capacity = max(2, 4 * lookups // devices)
    slots = devices * capacity
    vmem = pl.BlockSpec(memory_space=pltpu.VMEM)
    tiles = (lookups // LANES, LANES)
    return pl.pallas_call(
        functools.partial(send_kernel, dp, rows),
        name="send_gradients",
        out_shape=(
            jax.ShapeDtypeStruct((owned // 2, 2 * columns), jnp.float32),
            jax.ShapeDtypeStruct((devices, 1, 2 * capacity), jnp.int32),
            jax.ShapeDtypeStruct(tiles, jnp.int32),
        ),
        in_specs=[vmem] * 2,
        out_specs=(vmem,) * 3,
        scratch_shapes=[
            pltpu.VMEM((devices, 2 * capacity), jnp.int32),
            pltpu.VMEM((devices, 1, 2 * capacity), jnp.int32),
            pltpu.VMEM((slots, columns), jnp.bfloat16),
            pltpu.VMEM((slots, columns), jnp.bfloat16),
        ]
        + [pltpu.SemaphoreType.DMA((devices,))] * 4,
        compiler_params=pltpu.CompilerParams(
            collective_id=0, has_side_effects=True, vmem_limit_bytes=40 * 1024 * 1024
        ),
        cost_estimate=pl.CostEstimate(
            flops=400 * slots * owned * columns, bytes_accessed=owned * columns * 4, transcendentals=0
        ),
    )(
        jnp.stack([part.reshape(tiles) for part in (owners, offsets, next_owners, next_offsets)]),
        gradients,
    )


def update(acc_ref, embedding_ref, state_ref, new_state_ref, table):
    half = acc_ref.shape[0]
    eye = lax.broadcasted_iota(jnp.int32, (LANES, LANES), 0) == lax.broadcasted_iota(
        jnp.int32, (LANES, LANES), 1
    )
    ones = jnp.ones((2 * LANES, LANES), jnp.bfloat16)
    ones_row = jnp.ones((SUB, 2 * LANES), jnp.bfloat16)

    def split(x):
        high = x.astype(jnp.bfloat16)
        return high, (x - high.astype(jnp.float32)).astype(jnp.bfloat16)

    for side in range(table.shape[0] // half):

        @pl.loop(0, half // LANES, unroll=4)
        def _(step):
            tile = side * (half // LANES) + step
            span = pl.ds(pl.multiple_of(tile * LANES, LANES), LANES)
            low = pl.ds(pl.multiple_of(step * LANES, LANES), LANES)
            grad_sum = acc_ref[low, side * LANES : (side + 1) * LANES]
            square = jnp.concatenate(split(grad_sum * grad_sum), axis=1)
            mean = lax.dot_general(
                ones_row, square, (((1,), (1,)), ((), ())), preferred_element_type=jnp.float32
            )[0:1, :] * (1.0 / LANES)
            state = state_ref[pl.ds(tile, 1), :] + mean
            new_state_ref[pl.ds(tile, 1), :] = state
            scale = jnp.broadcast_to(0.5 * lax.rsqrt(state), (LANES, LANES))
            diagonal = jnp.concatenate(split(jnp.where(eye, scale, 0.0)), axis=1)
            rate = jnp.dot(diagonal, ones, preferred_element_type=jnp.float32)
            table[span, :] = embedding_ref[span, :] - grad_sum * rate


def fetch_kernel(
    dp, rows,
    wanted_hbm, place_ref, acc_ref, embedding_ref, state_ref,
    table, new_state_ref, next_ref,
    wanted_ref, picked, outgoing, incoming, place, total, wanted_sem, data_send, data_recv,
):
    devices = dp * rows
    slots = outgoing.shape[0]
    capacity = slots // devices
    group = 2 if capacity == LANES else 1
    depth = group * capacity

    greet(dp, rows)
    load = pltpu.make_async_copy(wanted_hbm, wanted_ref, wanted_sem)
    load.start()
    update(acc_ref, embedding_ref, state_ref, new_state_ref, table)
    load.wait()

    def copy(dz, dr):
        i = dz * rows + dr
        span = pl.ds(pl.multiple_of(i * capacity, capacity), capacity)
        return pltpu.make_async_remote_copy(
            src_ref=outgoing.at[span, :], dst_ref=incoming.at[span, :],
            send_sem=data_send.at[i], recv_sem=data_recv.at[i],
            device_id=peer(dp, rows, dz, dr), device_id_type=MESH,
        )

    def gather(i):
        start = pl.multiple_of(i * capacity, capacity)
        for k in range(capacity):
            picked[pl.ds(k, 1), :] = table[pl.ds(wanted_ref[start + k], 1), :]
        outgoing[pl.ds(start, capacity), :] = picked[...].astype(jnp.bfloat16)

    for position, dz in enumerate(plane_order(dp)):
        gather(dz * rows)
        if position == 0:
            gathered(dp, rows)

        @pl.loop(1, rows)
        def _(dr):
            gather(dz * rows + dr)
            if dz:
                copy(dz, dr - 1).start()
            else:
                pl.when(dr > 1)(lambda: copy(dz, dr - 1).start())

        copy(dz, rows - 1).start()

    incoming[0:capacity, :] = outgoing[0:capacity, :]
    total[...] = jnp.zeros(total.shape, jnp.float32)
    for b in range(place_ref.shape[0]):
        row = place_ref[b : b + 1, :].astype(jnp.float32)
        place[b * LANES : (b + 1) * LANES, :] = jnp.broadcast_to(row, (LANES, LANES)).T.astype(
            jnp.int32
        )

    lookups = total.shape[0]
    per_plane = rows // group
    for dz in plane_order(dp):

        @pl.loop(0, per_plane)
        def _(step):
            for k in range(group):
                dr = step * group + k

                def arrive():
                    copy(dz, dr).wait_recv()

                if dz == 0:
                    pl.when(dr > 0)(arrive)
                else:
                    arrive()
            start = pl.multiple_of((dz * per_plane + step) * depth, depth)
            lane = lax.broadcasted_iota(jnp.int32, (lookups, capacity), 1)
            chosen = jnp.concatenate(
                [
                    jnp.where(place[:, :capacity] == lane + (start + k * capacity), 1.0, 0.0)
                    for k in range(group)
                ],
                axis=1,
            ).astype(jnp.bfloat16)
            total[...] += jnp.dot(
                chosen, incoming[pl.ds(start, depth), :], preferred_element_type=jnp.float32
            )

    next_ref[...] = total[...].astype(jnp.bfloat16)

    for dz in plane_order(dp):

        @pl.loop(0 if dz else 1, rows)
        def _(dr):
            copy(dz, dr).wait_send()


def fetch(dp, rows, wanted, place, acc, embedding, state):
    slots = wanted.shape[0]
    devices = dp * rows
    lookups = place.shape[0] * place.shape[1]
    owned, columns = embedding.shape
    tiles = (owned // LANES, LANES)
    vmem = pl.BlockSpec(memory_space=pltpu.VMEM)
    hbm = pl.BlockSpec(memory_space=pltpu.HBM)
    table, new_state, next_rows = pl.pallas_call(
        functools.partial(fetch_kernel, dp, rows),
        name="fetch",
        out_shape=(
            jax.ShapeDtypeStruct((owned, columns), jnp.float32),
            jax.ShapeDtypeStruct(tiles, jnp.float32),
            jax.ShapeDtypeStruct((lookups, columns), jnp.bfloat16),
        ),
        in_specs=[hbm] + [vmem] * 4,
        out_specs=(vmem,) * 3,
        scratch_shapes=[
            pltpu.SMEM((slots,), jnp.int32),
            pltpu.VMEM((slots // devices, columns), jnp.float32),
            pltpu.VMEM((slots, columns), jnp.bfloat16),
            pltpu.VMEM((slots, columns), jnp.bfloat16),
            pltpu.VMEM((lookups, LANES), jnp.int32),
            pltpu.VMEM((lookups, columns), jnp.float32),
            pltpu.SemaphoreType.DMA,
            pltpu.SemaphoreType.DMA((devices,)),
            pltpu.SemaphoreType.DMA((devices,)),
        ],
        compiler_params=pltpu.CompilerParams(
            collective_id=1, has_side_effects=True, vmem_limit_bytes=40 * 1024 * 1024
        ),
    )(wanted, place, acc, embedding, state.reshape(tiles))
    return table, new_state.reshape(owned), next_rows


def on_device(owners, offsets, gradients, embedding, adagrad_state, next_owners, next_offsets):
    dp, rows = lax.axis_size("dp"), lax.axis_size("rows")
    acc, met, next_place = send_gradients(
        dp, rows, owners, offsets, next_owners, next_offsets, gradients, embedding.shape[0]
    )
    wanted = met[:, 0, met.shape[2] // 2 :].reshape(-1)
    new_embedding, new_state, next_rows = fetch(
        dp, rows, wanted, next_place, acc, embedding, adagrad_state
    )
    return (new_embedding, new_state, next_rows)


def solution(mesh):
    in_specs = (
        P(("dp", "rows"), None),
        P(("dp", "rows")),
        P(("dp", "rows"), None),
        P(("dp", "rows"), None),
        P(("dp", "rows")),
        P(("dp", "rows"), None),
        P(("dp", "rows")),
    )
    out_specs = (P(("dp", "rows"), None), P(("dp", "rows")), P(("dp", "rows"), None))
    return jax.shard_map(
        on_device, mesh=mesh, in_specs=in_specs, out_specs=out_specs, check_vma=False
    )
```

```python
import functools

import jax
import jax.numpy as jnp
from jax import lax
from jax.experimental import pallas as pl
from jax.experimental.pallas import tpu as pltpu
from jax.sharding import PartitionSpec as P

LANES = 128
SUB = 16
BASE = 256
MESH = pl.DeviceIdType.MESH


def flip(value, step, size):
    bit, result = 1, value
    while bit < size:
        own = lax.rem(lax.div(value, bit), 2)
        if isinstance(step, int):
            if step // bit % 2:
                result = result + bit * (1 - 2 * own)
        else:
            other = lax.rem(lax.div(step, bit), 2)
            result = result + bit * other * (1 - 2 * own)
        bit *= 2
    return result


def plane_order(dp):
    return [dp - 1] + list(range(dp - 1))


def peer(dp, rows, dz, dr):
    z, r = lax.axis_index("dp"), lax.axis_index("rows")
    return (flip(z, dz, dp), flip(r, dr, rows))


def greet(dp, rows):
    barrier = pltpu.get_barrier_semaphore()
    for i in range(1, dp * rows):
        pl.semaphore_signal(
            barrier, inc=1, device_id=peer(dp, rows, i // rows, i % rows), device_id_type=MESH
        )


def gathered(dp, rows):
    pl.semaphore_wait(pltpu.get_barrier_semaphore(), dp * rows - 1)


def selectors(names, count):
    shape = (SUB, names.shape[1])
    low = lax.broadcasted_iota(jnp.int32, shape, 0) == names % SUB
    ones = jnp.where(low, 1.0, 0.0).astype(jnp.bfloat16)
    high = jnp.broadcast_to((names // SUB).astype(jnp.float32), shape)

    def pick(start):
        shifted = (high - start).astype(jnp.bfloat16)
        zero = jnp.zeros(shape, jnp.bfloat16)
        return jnp.concatenate(
            [jnp.where(shifted == jnp.bfloat16(k), ones, zero) for k in range(count // SUB)], axis=0
        )

    return pick


def route(names, values, me, devices, capacity):
    blocks = names.shape[0]
    columns = names.shape[1]
    relative = jnp.bitwise_xor(names, me)
    index = lax.broadcasted_iota(jnp.int32, (devices, columns), 0)
    hits = [jnp.where(index == relative[b : b + 1, :], 1.0, 0.0) for b in range(blocks)]
    before = jnp.where(
        lax.broadcasted_iota(jnp.int32, (columns, columns), 0)
        < lax.broadcasted_iota(jnp.int32, (columns, columns), 1),
        1.0,
        0.0,
    ).astype(jnp.bfloat16)
    one_hot = [hit.astype(jnp.bfloat16) for hit in hits]
    ahead = jnp.dot(
        jnp.concatenate(one_hot, axis=0), before, preferred_element_type=jnp.float32
    )
    seen = jnp.zeros((devices, 1), jnp.float32)
    slots = []
    for b in range(blocks):
        within = ahead[b * devices : (b + 1) * devices, :] + seen
        slots.append(jnp.sum(hits[b] * within, axis=0, keepdims=True))
        seen = seen + jnp.sum(hits[b], axis=1, keepdims=True)
    slots = jnp.concatenate(slots, axis=0).astype(jnp.int32)
    high = (values // BASE).astype(jnp.float32)
    low = (values % BASE).astype(jnp.float32)
    place = lax.broadcasted_iota(jnp.int32, (capacity, columns), 0)
    marked = []
    for b in range(blocks):
        taken = place == slots[b : b + 1, :]
        marked.append(
            jnp.concatenate(
                [jnp.where(taken, high[b : b + 1, :], 0.0), jnp.where(taken, low[b : b + 1, :], 0.0)],
                axis=0,
            ).astype(jnp.bfloat16)
        )
    table = lax.dot_general(
        jnp.concatenate(one_hot, axis=1),
        jnp.concatenate(marked, axis=1),
        (((1,), (1,)), ((), ())),
        preferred_element_type=jnp.float32,
    )
    table = (table[:, :capacity] * BASE + table[:, capacity:]).astype(jnp.int32)
    return relative * capacity + slots, table


def send_kernel(
    dp, rows,
    index_ref, gradients_ref,
    acc_ref, met_ref, next_place_ref,
    flat, meta_ref, outgoing, incoming, meta_send, meta_recv, data_send, data_recv,
):
    devices = dp * rows
    slots = outgoing.shape[0]
    capacity = slots // devices
    columns = gradients_ref.shape[1]
    half = acc_ref.shape[0]
    group = 2 if capacity == LANES else 1
    depth = group * capacity

    greet(dp, rows)

    me = lax.axis_index("dp") * rows + lax.axis_index("rows")
    place, table = route(index_ref[0], index_ref[1], me, devices, capacity)
    next_place, next_table = route(index_ref[2], index_ref[3], me, devices, capacity)
    next_place_ref[...] = next_place
    flat[...] = jnp.concatenate([table, next_table], axis=1)
    for i in range(devices):
        meta_ref[i] = flat[i : i + 1, :]

    made = min(512, rows * capacity)
    pick = selectors(
        jnp.concatenate([place[b : b + 1, :] for b in range(place.shape[0])], axis=1), made
    )

    def copies(dz, dr):
        i = dz * rows + dr
        span = pl.ds(pl.multiple_of(i * capacity, capacity), capacity)
        to = peer(dp, rows, dz, dr)
        meta = pltpu.make_async_remote_copy(
            src_ref=meta_ref.at[i], dst_ref=met_ref.at[i],
            send_sem=meta_send.at[i], recv_sem=meta_recv.at[i],
            device_id=to, device_id_type=MESH,
        )
        data = pltpu.make_async_remote_copy(
            src_ref=outgoing.at[span, :], dst_ref=incoming.at[span, :],
            send_sem=data_send.at[i], recv_sem=data_recv.at[i],
            device_id=to, device_id_type=MESH,
        )
        return meta, data

    plane = rows * capacity
    for position, dz in enumerate(plane_order(dp)):

        @pl.loop(dz * plane // made, (dz + 1) * plane // made)
        def _(step):
            start = pl.multiple_of(step * made, made)
            outgoing[pl.ds(start, made), :] = jnp.dot(
                pick((step * (made // SUB)).astype(jnp.float32)),
                gradients_ref[...],
                preferred_element_type=jnp.float32,
            ).astype(jnp.bfloat16)

        if position == 0:
            gathered(dp, rows)

        for dr in range(0 if dz else 1, rows):
            meta, data = copies(dz, dr)
            meta.start()
            data.start()

    @pl.loop(0, half // LANES)
    def _(step):
        acc_ref[pl.ds(pl.multiple_of(step * LANES, LANES), LANES), :] = jnp.zeros(
            (LANES, acc_ref.shape[1]), jnp.float32
        )

    met_ref[0] = meta_ref[0]
    incoming[0:capacity, :] = outgoing[0:capacity, :]

    chunk = min(1024, half)

    def accumulate(tile):
        met = [met_ref[tile * group + k][:, :capacity] for k in range(group)]
        parts = []
        for k in range(group):
            side = jnp.broadcast_to((met[k] // half).astype(jnp.float32), (columns, capacity)).T
            start = pl.multiple_of((tile * group + k) * capacity, capacity)
            block = incoming[pl.ds(start, capacity), :].astype(jnp.float32)
            parts.append(
                jnp.concatenate(
                    [jnp.where(side > 0.5, 0.0, block), jnp.where(side > 0.5, block, 0.0)], axis=1
                ).astype(jnp.bfloat16)
            )
        wide = jnp.concatenate(parts, axis=0) if group > 1 else parts[0]
        names = (jnp.concatenate(met, axis=1) if group > 1 else met[0]) % half
        pick_rows = selectors(names, chunk)

        @pl.loop(0, half // chunk)
        def _(step):
            span = pl.ds(pl.multiple_of(step * chunk, chunk), chunk)
            acc_ref[span, :] += jnp.dot(
                pick_rows((step * (chunk // SUB)).astype(jnp.float32)),
                wide,
                preferred_element_type=jnp.float32,
            )

    per_plane = rows // group
    for dz in plane_order(dp):

        @pl.loop(0, per_plane)
        def _(step):
            for k in range(group):
                dr = step * group + k

                def arrive():
                    meta, data = copies(dz, dr)
                    meta.wait_recv()
                    data.wait_recv()

                if dz == 0:
                    pl.when(dr > 0)(arrive)
                else:
                    arrive()
            accumulate(dz * per_plane + step)

    for dz in plane_order(dp):

        @pl.loop(0 if dz else 1, rows)
        def _(dr):
            meta, data = copies(dz, dr)
            meta.wait_send()
            data.wait_send()


def send_gradients(dp, rows, owners, offsets, next_owners, next_offsets, gradients, owned):
    devices = dp * rows
    lookups, columns = gradients.shape
    capacity = max(2, 4 * lookups // devices)
    slots = devices * capacity
    vmem = pl.BlockSpec(memory_space=pltpu.VMEM)
    tiles = (lookups // LANES, LANES)
    return pl.pallas_call(
        functools.partial(send_kernel, dp, rows),
        name="send_gradients",
        out_shape=(
            jax.ShapeDtypeStruct((owned // 2, 2 * columns), jnp.float32),
            jax.ShapeDtypeStruct((devices, 1, 2 * capacity), jnp.int32),
            jax.ShapeDtypeStruct(tiles, jnp.int32),
        ),
        in_specs=[vmem] * 2,
        out_specs=(vmem,) * 3,
        scratch_shapes=[
            pltpu.VMEM((devices, 2 * capacity), jnp.int32),
            pltpu.VMEM((devices, 1, 2 * capacity), jnp.int32),
            pltpu.VMEM((slots, columns), jnp.bfloat16),
            pltpu.VMEM((slots, columns), jnp.bfloat16),
        ]
        + [pltpu.SemaphoreType.DMA((devices,))] * 4,
        compiler_params=pltpu.CompilerParams(
            collective_id=0, has_side_effects=True, vmem_limit_bytes=40 * 1024 * 1024
        ),
        cost_estimate=pl.CostEstimate(
            flops=400 * slots * owned * columns, bytes_accessed=owned * columns * 4, transcendentals=0
        ),
    )(
        jnp.stack([part.reshape(tiles) for part in (owners, offsets, next_owners, next_offsets)]),
        gradients,
    )


def split(x):
    high = x.astype(jnp.bfloat16)
    return high, (x - high.astype(jnp.float32)).astype(jnp.bfloat16)


def update(acc_ref, embedding_ref, state_ref, new_state_ref, rate_ref, table):
    half = acc_ref.shape[0]
    tiles = half // LANES
    eye = lax.broadcasted_iota(jnp.int32, (LANES, LANES), 0) == lax.broadcasted_iota(
        jnp.int32, (LANES, LANES), 1
    )
    same = jnp.where(eye, 1.0, 0.0).astype(jnp.bfloat16)
    ones = jnp.ones((2 * LANES, LANES), jnp.bfloat16)
    sides = table.shape[0] // half

    batch = min(8, tiles)

    for side in range(sides):

        @pl.loop(0, tiles // batch)
        def _(step):
            low = pl.ds(pl.multiple_of(step * batch * LANES, batch * LANES), batch * LANES)
            grad_sum = acc_ref[low, side * LANES : (side + 1) * LANES]
            square = jnp.concatenate(split(grad_sum * grad_sum), axis=1)
            sums = jnp.dot(square, ones, preferred_element_type=jnp.float32)
            means = [
                jnp.sum(
                    jnp.where(eye, sums[k * LANES : (k + 1) * LANES, :], 0.0), axis=0, keepdims=True
                )
                for k in range(batch)
            ]
            first = pl.multiple_of(side * tiles + step * batch, batch)
            rate_ref[pl.ds(first, batch), :] = jnp.concatenate(means, axis=0)

    state = state_ref[...] + rate_ref[...] * (1.0 / LANES)
    new_state_ref[...] = state
    rate_ref[...] = 0.5 * lax.rsqrt(state)

    for side in range(sides):

        @pl.loop(0, tiles // batch)
        def _(step):
            first = pl.multiple_of(side * tiles + step * batch, batch)
            rows = batch * LANES
            span = pl.ds(pl.multiple_of(first * LANES, rows), rows)
            low = pl.ds(pl.multiple_of(step * rows, rows), rows)
            parts = split(rate_ref[pl.ds(first, batch), :])
            diagonal = jnp.concatenate(
                [
                    jnp.concatenate([same * part[k : k + 1, :] for part in parts], axis=1)
                    for k in range(batch)
                ],
                axis=0,
            )
            rate = jnp.dot(diagonal, ones, preferred_element_type=jnp.float32)
            grad_sum = acc_ref[low, side * LANES : (side + 1) * LANES]
            table[span, :] = embedding_ref[span, :] - grad_sum * rate


def fetch_kernel(
    dp, rows,
    wanted_hbm, place_ref, acc_ref, embedding_ref, state_ref,
    table, new_state_ref, next_ref,
    wanted_ref, picked, outgoing, incoming, place, total, rate_ref, wanted_sem, data_send, data_recv,
):
    devices = dp * rows
    slots = outgoing.shape[0]
    capacity = slots // devices
    group = 2 if capacity == LANES else 1
    depth = group * capacity

    greet(dp, rows)
    load = pltpu.make_async_copy(wanted_hbm, wanted_ref, wanted_sem)
    load.start()
    update(acc_ref, embedding_ref, state_ref, new_state_ref, rate_ref, table)
    load.wait()

    def copy(dz, dr):
        i = dz * rows + dr
        span = pl.ds(pl.multiple_of(i * capacity, capacity), capacity)
        return pltpu.make_async_remote_copy(
            src_ref=outgoing.at[span, :], dst_ref=incoming.at[span, :],
            send_sem=data_send.at[i], recv_sem=data_recv.at[i],
            device_id=peer(dp, rows, dz, dr), device_id_type=MESH,
        )

    def gather(i):
        start = pl.multiple_of(i * capacity, capacity)
        for k in range(capacity):
            picked[pl.ds(k, 1), :] = table[pl.ds(wanted_ref[start + k], 1), :]
        outgoing[pl.ds(start, capacity), :] = picked[...].astype(jnp.bfloat16)

    for position, dz in enumerate(plane_order(dp)):
        gather(dz * rows)
        if position == 0:
            gathered(dp, rows)

        @pl.loop(1, rows)
        def _(dr):
            gather(dz * rows + dr)
            if dz:
                copy(dz, dr - 1).start()
            else:
                pl.when(dr > 1)(lambda: copy(dz, dr - 1).start())

        copy(dz, rows - 1).start()

    incoming[0:capacity, :] = outgoing[0:capacity, :]
    total[...] = jnp.zeros(total.shape, jnp.float32)
    for b in range(place_ref.shape[0]):
        row = place_ref[b : b + 1, :].astype(jnp.float32)
        place[b * LANES : (b + 1) * LANES, :] = jnp.broadcast_to(row, (LANES, LANES)).T.astype(
            jnp.int32
        )

    lookups = total.shape[0]
    per_plane = rows // group
    for dz in plane_order(dp):

        @pl.loop(0, per_plane)
        def _(step):
            for k in range(group):
                dr = step * group + k

                def arrive():
                    copy(dz, dr).wait_recv()

                if dz == 0:
                    pl.when(dr > 0)(arrive)
                else:
                    arrive()
            start = pl.multiple_of((dz * per_plane + step) * depth, depth)
            lane = lax.broadcasted_iota(jnp.int32, (lookups, capacity), 1)
            chosen = jnp.concatenate(
                [
                    jnp.where(place[:, :capacity] == lane + (start + k * capacity), 1.0, 0.0)
                    for k in range(group)
                ],
                axis=1,
            ).astype(jnp.bfloat16)
            total[...] += jnp.dot(
                chosen, incoming[pl.ds(start, depth), :], preferred_element_type=jnp.float32
            )

    next_ref[...] = total[...].astype(jnp.bfloat16)

    for dz in plane_order(dp):

        @pl.loop(0 if dz else 1, rows)
        def _(dr):
            copy(dz, dr).wait_send()


def finish_kernel(*refs):
    count = len(refs) // 2
    sems = refs[-1]
    copies = []
    for source, target in zip(refs[:count], refs[count:-1]):
        pieces = 8 if source.shape[0] > 4096 else 1
        size = source.shape[0] // pieces
        for piece in range(pieces):
            span = pl.ds(piece * size, size)
            copies.append(
                pltpu.make_async_copy(
                    source.at[span, :], target.at[span, :], sems.at[len(copies)]
                )
            )
            copies[-1].start()
    for copy in copies:
        copy.wait()


def finish(*arrays):
    vmem = pl.BlockSpec(memory_space=pltpu.VMEM)
    hbm = pl.BlockSpec(memory_space=pltpu.HBM)
    return pl.pallas_call(
        finish_kernel,
        name="finish",
        out_shape=tuple(jax.ShapeDtypeStruct(array.shape, array.dtype) for array in arrays),
        in_specs=[vmem] * len(arrays),
        out_specs=(hbm,) * len(arrays),
        scratch_shapes=[pltpu.SemaphoreType.DMA((8 + len(arrays),))],
        compiler_params=pltpu.CompilerParams(vmem_limit_bytes=16 * 1024 * 1024),
    )(*arrays)


def fetch(dp, rows, wanted, place, acc, embedding, state):
    slots = wanted.shape[0]
    devices = dp * rows
    lookups = place.shape[0] * place.shape[1]
    owned, columns = embedding.shape
    tiles = (owned // LANES, LANES)
    vmem = pl.BlockSpec(memory_space=pltpu.VMEM)
    hbm = pl.BlockSpec(memory_space=pltpu.HBM)
    table, new_state, next_rows = pl.pallas_call(
        functools.partial(fetch_kernel, dp, rows),
        name="fetch",
        out_shape=(
            jax.ShapeDtypeStruct((owned, columns), jnp.float32),
            jax.ShapeDtypeStruct(tiles, jnp.float32),
            jax.ShapeDtypeStruct((lookups, columns), jnp.bfloat16),
        ),
        in_specs=[hbm] + [vmem] * 4,
        out_specs=(vmem,) * 3,
        scratch_shapes=[
            pltpu.SMEM((slots,), jnp.int32),
            pltpu.VMEM((slots // devices, columns), jnp.float32),
            pltpu.VMEM((slots, columns), jnp.bfloat16),
            pltpu.VMEM((slots, columns), jnp.bfloat16),
            pltpu.VMEM((lookups, LANES), jnp.int32),
            pltpu.VMEM((lookups, columns), jnp.float32),
            pltpu.VMEM(tiles, jnp.float32),
            pltpu.SemaphoreType.DMA,
            pltpu.SemaphoreType.DMA((devices,)),
            pltpu.SemaphoreType.DMA((devices,)),
        ],
        compiler_params=pltpu.CompilerParams(
            collective_id=1, has_side_effects=True, vmem_limit_bytes=40 * 1024 * 1024
        ),
    )(wanted, place, acc, embedding, state.reshape(tiles))
    new_embedding, new_state, next_rows = finish(table, new_state, next_rows)
    return new_embedding, new_state.reshape(owned), next_rows


def on_device(owners, offsets, gradients, embedding, adagrad_state, next_owners, next_offsets):
    dp, rows = lax.axis_size("dp"), lax.axis_size("rows")
    acc, met, next_place = send_gradients(
        dp, rows, owners, offsets, next_owners, next_offsets, gradients, embedding.shape[0]
    )
    wanted = met[:, 0, met.shape[2] // 2 :].reshape(-1)
    new_embedding, new_state, next_rows = fetch(
        dp, rows, wanted, next_place, acc, embedding, adagrad_state
    )
    return (new_embedding, new_state, next_rows)


def solution(mesh):
    in_specs = (
        P(("dp", "rows"), None),
        P(("dp", "rows")),
        P(("dp", "rows"), None),
        P(("dp", "rows"), None),
        P(("dp", "rows")),
        P(("dp", "rows"), None),
        P(("dp", "rows")),
    )
    out_specs = (P(("dp", "rows"), None), P(("dp", "rows")), P(("dp", "rows"), None))
    return jax.shard_map(
        on_device, mesh=mesh, in_specs=in_specs, out_specs=out_specs, check_vma=False
    )
```

```python
import functools

import jax
import jax.numpy as jnp
from jax import lax
from jax.experimental import pallas as pl
from jax.experimental.pallas import tpu as pltpu
from jax.sharding import PartitionSpec as P

LANES = 128
SUB = 16
BASE = 256
MESH = pl.DeviceIdType.MESH


def flip(value, step, size):
    bit, result = 1, value
    while bit < size:
        own = lax.rem(lax.div(value, bit), 2)
        if isinstance(step, int):
            if step // bit % 2:
                result = result + bit * (1 - 2 * own)
        else:
            other = lax.rem(lax.div(step, bit), 2)
            result = result + bit * other * (1 - 2 * own)
        bit *= 2
    return result


def is_inner(dp):
    return lax.rem(lax.div(lax.axis_index("dp") + 1, 2), 2)


def peer(dp, rows, dz, dr):
    z, r = lax.axis_index("dp"), lax.axis_index("rows")
    return (flip(z, dz, dp), flip(r, dr, rows))


def greet(dp, rows):
    barrier = pltpu.get_barrier_semaphore()
    for i in range(1, dp * rows):
        pl.semaphore_signal(
            barrier, inc=1, device_id=peer(dp, rows, i // rows, i % rows), device_id_type=MESH
        )


def gathered(dp, rows):
    pl.semaphore_wait(pltpu.get_barrier_semaphore(), dp * rows - 1)


def selectors(names, count):
    shape = (SUB, names.shape[1])
    low = lax.broadcasted_iota(jnp.int32, shape, 0) == names % SUB
    ones = jnp.where(low, 1.0, 0.0).astype(jnp.bfloat16)
    high = jnp.broadcast_to((names // SUB).astype(jnp.float32), shape)

    def pick(start):
        shifted = (high - start).astype(jnp.bfloat16)
        zero = jnp.zeros(shape, jnp.bfloat16)
        return jnp.concatenate(
            [jnp.where(shifted == jnp.bfloat16(k), ones, zero) for k in range(count // SUB)], axis=0
        )

    return pick


def route(names, values, me, devices, capacity):
    blocks = names.shape[0]
    columns = names.shape[1]
    relative = jnp.bitwise_xor(names, me)
    index = lax.broadcasted_iota(jnp.int32, (devices, columns), 0)
    hits = [jnp.where(index == relative[b : b + 1, :], 1.0, 0.0) for b in range(blocks)]
    before = jnp.where(
        lax.broadcasted_iota(jnp.int32, (columns, columns), 0)
        < lax.broadcasted_iota(jnp.int32, (columns, columns), 1),
        1.0,
        0.0,
    ).astype(jnp.bfloat16)
    one_hot = [hit.astype(jnp.bfloat16) for hit in hits]
    ahead = jnp.dot(
        jnp.concatenate(one_hot, axis=0), before, preferred_element_type=jnp.float32
    )
    seen = jnp.zeros((devices, 1), jnp.float32)
    slots = []
    for b in range(blocks):
        within = ahead[b * devices : (b + 1) * devices, :] + seen
        slots.append(jnp.sum(hits[b] * within, axis=0, keepdims=True))
        seen = seen + jnp.sum(hits[b], axis=1, keepdims=True)
    slots = jnp.concatenate(slots, axis=0).astype(jnp.int32)
    high = (values // BASE).astype(jnp.float32)
    low = (values % BASE).astype(jnp.float32)
    place = lax.broadcasted_iota(jnp.int32, (capacity, columns), 0)
    marked = []
    for b in range(blocks):
        taken = place == slots[b : b + 1, :]
        marked.append(
            jnp.concatenate(
                [jnp.where(taken, high[b : b + 1, :], 0.0), jnp.where(taken, low[b : b + 1, :], 0.0)],
                axis=0,
            ).astype(jnp.bfloat16)
        )
    table = lax.dot_general(
        jnp.concatenate(one_hot, axis=1),
        jnp.concatenate(marked, axis=1),
        (((1,), (1,)), ((), ())),
        preferred_element_type=jnp.float32,
    )
    table = (table[:, :capacity] * BASE + table[:, capacity:]).astype(jnp.int32)
    return relative * capacity + slots, table


def send_kernel(
    dp, rows,
    index_ref, gradients_ref,
    acc_ref, met_ref, places_ref, relayed_ref,
    flat, meta_ref, outgoing, incoming, raw, relay_out,
    meta_send, meta_recv, data_send, data_recv, relay_send, raw_sems,
):
    devices = dp * rows
    slots = outgoing.shape[0]
    capacity = slots // devices
    columns = gradients_ref.shape[1]
    half = acc_ref.shape[0]
    group = 2 if capacity == LANES else 1
    depth = group * capacity

    greet(dp, rows)

    me = lax.axis_index("dp") * rows + lax.axis_index("rows")
    place, table = route(index_ref[0], index_ref[1], me, devices, capacity)
    next_place, next_table = route(index_ref[2], index_ref[3], me, devices, capacity)
    places_ref[0] = place
    places_ref[1] = next_place
    flat[...] = jnp.concatenate([table, next_table], axis=1)
    for i in range(devices):
        meta_ref[i] = flat[i : i + 1, :]

    inner = is_inner(dp)
    plane = rows * capacity
    made = min(512, plane)

    def builder(place):
        return selectors(
            jnp.concatenate([place[b : b + 1, :] for b in range(place.shape[0])], axis=1), made
        )

    def build(pick, source, target, dz, base):
        @pl.loop(0, plane // made)
        def _(step):
            first = dz * plane + step * made
            target[pl.ds(pl.multiple_of(first - base, made), made), :] = jnp.dot(
                pick(jnp.float32(first // SUB) if isinstance(first, int)
                     else (first // SUB).astype(jnp.float32)),
                source[...],
                preferred_element_type=jnp.float32,
            ).astype(jnp.bfloat16)

    def span_of(i):
        return pl.ds(pl.multiple_of(i * capacity, capacity), capacity)

    def send_meta(dz, dr):
        i = dz * rows + dr
        return pltpu.make_async_remote_copy(
            src_ref=meta_ref.at[i], dst_ref=met_ref.at[i],
            send_sem=meta_send.at[i], recv_sem=meta_recv.at[i],
            device_id=peer(dp, rows, dz, dr), device_id_type=MESH,
        )

    def send_data(dz, dr):
        i = dz * rows + dr
        return pltpu.make_async_remote_copy(
            src_ref=outgoing.at[span_of(i), :], dst_ref=incoming.at[span_of(i), :],
            send_sem=data_send.at[i], recv_sem=data_recv.at[i],
            device_id=peer(dp, rows, dz, dr), device_id_type=MESH,
        )

    def relay_data(dz, dr):
        i = dz * rows + dr
        k = i - 2 * rows
        return pltpu.make_async_remote_copy(
            src_ref=relay_out.at[span_of(k), :], dst_ref=incoming.at[span_of(i), :],
            send_sem=relay_send.at[k], recv_sem=data_recv.at[i],
            device_id=peer(dp, rows, dz - 2, dr), device_id_type=MESH,
        )

    def send_raw():
        to = peer(dp, rows, 2, 0)
        return (
            pltpu.make_async_remote_copy(
                src_ref=places_ref, dst_ref=relayed_ref,
                send_sem=raw_sems.at[0], recv_sem=raw_sems.at[1],
                device_id=to, device_id_type=MESH,
            ),
            pltpu.make_async_remote_copy(
                src_ref=gradients_ref, dst_ref=raw,
                send_sem=raw_sems.at[2], recv_sem=raw_sems.at[3],
                device_id=to, device_id_type=MESH,
            ),
        )

    pick = builder(place)

    @pl.when(inner == 1)
    def _():
        build(pick, gradients_ref, outgoing, 2, 0)

    gathered(dp, rows)

    @pl.when(inner == 0)
    def _():
        for copy in send_raw():
            copy.start()

    for dz in (2, 1, 3, 0):
        for dr in range(0 if dz else 1, rows):
            send_meta(dz, dr).start()

    def send_plane(dz):
        for dr in range(0 if dz else 1, rows):
            send_data(dz, dr).start()

    @pl.when(inner == 1)
    def _():
        send_plane(2)

    build(pick, gradients_ref, outgoing, 1, 0)
    send_plane(1)

    @pl.when(inner == 1)
    def _():
        build(pick, gradients_ref, outgoing, 3, 0)
        send_plane(3)

    build(pick, gradients_ref, outgoing, 0, 0)
    send_plane(0)

    @pl.loop(0, half // LANES)
    def _(step):
        acc_ref[pl.ds(pl.multiple_of(step * LANES, LANES), LANES), :] = jnp.zeros(
            (LANES, acc_ref.shape[1]), jnp.float32
        )

    met_ref[0] = meta_ref[0]
    incoming[0:capacity, :] = outgoing[0:capacity, :]

    chunk = min(1024, half)

    def accumulate(tile):
        met = [met_ref[tile * group + k][:, :capacity] for k in range(group)]
        parts = []
        for k in range(group):
            side = jnp.broadcast_to((met[k] // half).astype(jnp.float32), (columns, capacity)).T
            start = pl.multiple_of((tile * group + k) * capacity, capacity)
            block = incoming[pl.ds(start, capacity), :].astype(jnp.float32)
            parts.append(
                jnp.concatenate(
                    [jnp.where(side > 0.5, 0.0, block), jnp.where(side > 0.5, block, 0.0)], axis=1
                ).astype(jnp.bfloat16)
            )
        wide = jnp.concatenate(parts, axis=0) if group > 1 else parts[0]
        names = (jnp.concatenate(met, axis=1) if group > 1 else met[0]) % half
        pick_rows = selectors(names, chunk)

        @pl.loop(0, half // chunk)
        def _(step):
            span = pl.ds(pl.multiple_of(step * chunk, chunk), chunk)
            acc_ref[span, :] += jnp.dot(
                pick_rows((step * (chunk // SUB)).astype(jnp.float32)),
                wide,
                preferred_element_type=jnp.float32,
            )

    per_plane = rows // group

    def take_plane(dz):
        @pl.loop(0, per_plane)
        def _(step):
            for k in range(group):
                dr = step * group + k

                def arrive_meta():
                    send_meta(dz, dr).wait_recv()

                def arrive():
                    send_data(dz, dr).wait_recv()

                if dz == 0:
                    pl.when(dr > 0)(arrive_meta)
                    pl.when(dr > 0)(arrive)
                elif dz == 2:
                    arrive_meta()
                    pl.when(dr + (1 - inner) > 0)(arrive)
                else:
                    arrive_meta()
                    arrive()
            accumulate(dz * per_plane + step)

    take_plane(0)
    take_plane(1)

    @pl.when(inner == 1)
    def _():
        for copy in send_raw():
            copy.wait_recv()
        relay_pick = builder(relayed_ref[0])
        for dz in (3, 2):
            build(relay_pick, raw, relay_out, dz, 2 * plane)
            for dr in range(0 if dz == 3 else 1, rows):
                relay_data(dz, dr).start()
        incoming[2 * plane : 2 * plane + capacity, :] = relay_out[0:capacity, :]

    take_plane(2)
    take_plane(3)

    for dz in range(dp):

        @pl.loop(0 if dz else 1, rows)
        def _(dr):
            send_meta(dz, dr).wait_send()
            if dz < 2:
                send_data(dz, dr).wait_send()

    @pl.when(inner == 1)
    def _():
        for dz in (2, 3):

            @pl.loop(0, rows)
            def _(dr):
                send_data(dz, dr).wait_send()

            @pl.loop(0 if dz == 3 else 1, rows)
            def _(dr):
                relay_data(dz, dr).wait_send()

    @pl.when(inner == 0)
    def _():
        for copy in send_raw():
            copy.wait_send()


def send_gradients(dp, rows, owners, offsets, next_owners, next_offsets, gradients, owned):
    devices = dp * rows
    lookups, columns = gradients.shape
    capacity = max(2, 4 * lookups // devices)
    slots = devices * capacity
    vmem = pl.BlockSpec(memory_space=pltpu.VMEM)
    tiles = (lookups // LANES, LANES)
    return pl.pallas_call(
        functools.partial(send_kernel, dp, rows),
        name="send_gradients",
        out_shape=(
            jax.ShapeDtypeStruct((owned // 2, 2 * columns), jnp.float32),
            jax.ShapeDtypeStruct((devices, 1, 2 * capacity), jnp.int32),
            jax.ShapeDtypeStruct((2,) + tiles, jnp.int32),
            jax.ShapeDtypeStruct((2,) + tiles, jnp.int32),
        ),
        in_specs=[vmem] * 2,
        out_specs=(vmem,) * 4,
        scratch_shapes=[
            pltpu.VMEM((devices, 2 * capacity), jnp.int32),
            pltpu.VMEM((devices, 1, 2 * capacity), jnp.int32),
            pltpu.VMEM((slots, columns), jnp.bfloat16),
            pltpu.VMEM((slots, columns), jnp.bfloat16),
            pltpu.VMEM((lookups, columns), jnp.bfloat16),
            pltpu.VMEM((2 * rows * capacity, columns), jnp.bfloat16),
        ]
        + [pltpu.SemaphoreType.DMA((devices,))] * 4
        + [pltpu.SemaphoreType.DMA((2 * rows,)), pltpu.SemaphoreType.DMA((4,))],
        compiler_params=pltpu.CompilerParams(
            collective_id=0, has_side_effects=True, vmem_limit_bytes=40 * 1024 * 1024
        ),
        cost_estimate=pl.CostEstimate(
            flops=400 * slots * owned * columns, bytes_accessed=owned * columns * 4, transcendentals=0
        ),
    )(
        jnp.stack([part.reshape(tiles) for part in (owners, offsets, next_owners, next_offsets)]),
        gradients,
    )


def split(x):
    high = x.astype(jnp.bfloat16)
    return high, (x - high.astype(jnp.float32)).astype(jnp.bfloat16)


def update(acc_ref, embedding_ref, state_ref, new_state_ref, rate_ref, table):
    half = acc_ref.shape[0]
    tiles = half // LANES
    eye = lax.broadcasted_iota(jnp.int32, (LANES, LANES), 0) == lax.broadcasted_iota(
        jnp.int32, (LANES, LANES), 1
    )
    same = jnp.where(eye, 1.0, 0.0).astype(jnp.bfloat16)
    ones = jnp.ones((2 * LANES, LANES), jnp.bfloat16)
    sides = table.shape[0] // half

    batch = min(8, tiles)

    for side in range(sides):

        @pl.loop(0, tiles // batch)
        def _(step):
            low = pl.ds(pl.multiple_of(step * batch * LANES, batch * LANES), batch * LANES)
            grad_sum = acc_ref[low, side * LANES : (side + 1) * LANES]
            square = jnp.concatenate(split(grad_sum * grad_sum), axis=1)
            sums = jnp.dot(square, ones, preferred_element_type=jnp.float32)
            means = [
                jnp.sum(
                    jnp.where(eye, sums[k * LANES : (k + 1) * LANES, :], 0.0), axis=0, keepdims=True
                )
                for k in range(batch)
            ]
            first = pl.multiple_of(side * tiles + step * batch, batch)
            rate_ref[pl.ds(first, batch), :] = jnp.concatenate(means, axis=0)

    state = state_ref[...] + rate_ref[...] * (1.0 / LANES)
    new_state_ref[...] = state
    rate_ref[...] = 0.5 * lax.rsqrt(state)

    for side in range(sides):

        @pl.loop(0, tiles // batch)
        def _(step):
            first = pl.multiple_of(side * tiles + step * batch, batch)
            rows = batch * LANES
            span = pl.ds(pl.multiple_of(first * LANES, rows), rows)
            low = pl.ds(pl.multiple_of(step * rows, rows), rows)
            parts = split(rate_ref[pl.ds(first, batch), :])
            diagonal = jnp.concatenate(
                [
                    jnp.concatenate([same * part[k : k + 1, :] for part in parts], axis=1)
                    for k in range(batch)
                ],
                axis=0,
            )
            rate = jnp.dot(diagonal, ones, preferred_element_type=jnp.float32)
            grad_sum = acc_ref[low, side * LANES : (side + 1) * LANES]
            table[span, :] = embedding_ref[span, :] - grad_sum * rate


def fetch_kernel(
    dp, rows,
    wanted_hbm, places_ref, relayed_ref, acc_ref, embedding_ref, state_ref,
    table, new_state_ref, next_ref,
    wanted_ref, picked, outgoing, incoming, relay_in, place, total, partial, summed, rate_ref,
    wanted_sem, data_send, data_recv, relay_recv, raw_sems,
):
    devices = dp * rows
    slots = outgoing.shape[0]
    capacity = slots // devices
    group = 2 if capacity == LANES else 1
    depth = group * capacity

    greet(dp, rows)
    load = pltpu.make_async_copy(wanted_hbm, wanted_ref, wanted_sem)
    load.start()
    update(acc_ref, embedding_ref, state_ref, new_state_ref, rate_ref, table)
    load.wait()

    inner = is_inner(dp)
    plane = rows * capacity
    z, r = lax.axis_index("dp"), lax.axis_index("rows")

    def span_of(i):
        return pl.ds(pl.multiple_of(i * capacity, capacity), capacity)

    def answer(dz, dr):
        i = dz * rows + dr
        return pltpu.make_async_remote_copy(
            src_ref=outgoing.at[span_of(i), :], dst_ref=incoming.at[span_of(i), :],
            send_sem=data_send.at[i], recv_sem=data_recv.at[i],
            device_id=peer(dp, rows, dz, dr), device_id_type=MESH,
        )

    def relay(dr, side):
        i = (3 - inner) * rows + dr
        k = side * rows + dr
        return pltpu.make_async_remote_copy(
            src_ref=outgoing.at[span_of(i), :], dst_ref=relay_in.at[span_of(k), :],
            send_sem=data_send.at[i], recv_sem=relay_recv.at[k],
            device_id=(z + (1 - inner) * (1 - 2 * lax.rem(z, 2)), flip(r, dr, rows)),
            device_id_type=MESH,
        )

    def send_raw():
        return pltpu.make_async_remote_copy(
            src_ref=summed, dst_ref=partial, send_sem=raw_sems.at[0], recv_sem=raw_sems.at[1],
            device_id=peer(dp, rows, 2, 0), device_id_type=MESH,
        )

    def gather(i):
        start = pl.multiple_of(i * capacity, capacity)
        for k in range(capacity):
            picked[pl.ds(k, 1), :] = table[pl.ds(wanted_ref[start + k], 1), :]
        outgoing[pl.ds(start, capacity), :] = picked[...].astype(jnp.bfloat16)

    first, second = 3 - inner, 2 + inner
    gather(first * rows)
    gathered(dp, rows)
    side = 1 - inner

    @pl.loop(1, rows)
    def _(dr):
        gather(first * rows + dr)
        pl.when(dr + side > 1)(lambda: relay(dr - 1, side).start())

    relay(rows - 1, side).start()

    for dz in (second, 1, 0):
        gather(dz * rows)

        @pl.loop(1, rows)
        def _(dr):
            gather(dz * rows + dr)
            if isinstance(dz, int) and dz == 0:
                pl.when(dr > 1)(lambda: answer(dz, dr - 1).start())
            else:
                answer(dz, dr - 1).start()

        answer(dz, rows - 1).start()

    lookups = total.shape[0]
    per_plane = rows // group

    def turn(source):
        for b in range(source.shape[0]):
            row = source[b : b + 1, :].astype(jnp.float32)
            place[b * LANES : (b + 1) * LANES, :] = jnp.broadcast_to(row, (LANES, LANES)).T.astype(
                jnp.int32
            )
        total[...] = jnp.zeros(total.shape, jnp.float32)

    def put(base, blocks, start):
        lane = lax.broadcasted_iota(jnp.int32, (lookups, capacity), 1)
        chosen = jnp.concatenate(
            [
                jnp.where(place[:, :capacity] == lane + (base + start + k * capacity), 1.0, 0.0)
                for k in range(group)
            ],
            axis=1,
        ).astype(jnp.bfloat16)
        total[...] += jnp.dot(
            chosen, blocks[pl.ds(start, depth), :], preferred_element_type=jnp.float32
        )

    @pl.when(inner == 1)
    def _():
        relay_in[0:capacity, :] = outgoing[2 * plane : 2 * plane + capacity, :]
        turn(relayed_ref[1])
        for half in range(2):

            @pl.loop(0, per_plane)
            def _(step):
                for k in range(group):
                    dr = step * group + k

                    def arrive():
                        relay(dr, half).wait_recv()

                    if half == 0:
                        pl.when(dr > 0)(arrive)
                    else:
                        arrive()
                start = half * plane + step * depth
                put(2 * plane, relay_in, pl.multiple_of(start, depth))

        summed[...] = total[...].astype(jnp.bfloat16)

    turn(places_ref[1])

    @pl.when(inner == 1)
    def _():
        send_raw().start()

    incoming[0:capacity, :] = outgoing[0:capacity, :]

    def take_plane(dz):
        @pl.loop(0, per_plane)
        def _(step):
            for k in range(group):
                dr = step * group + k

                def arrive():
                    answer(dz, dr).wait_recv()

                if dz == 0:
                    pl.when(dr > 0)(arrive)
                else:
                    arrive()
            put(0, incoming, pl.multiple_of(dz * plane + step * depth, depth))

    take_plane(0)
    take_plane(1)

    @pl.when(inner == 1)
    def _():
        take_plane(2)
        take_plane(3)
        next_ref[...] = total[...].astype(jnp.bfloat16)
        send_raw().wait_send()

    @pl.when(inner == 0)
    def _():
        send_raw().wait_recv()
        next_ref[...] = (total[...] + partial[...].astype(jnp.float32)).astype(jnp.bfloat16)

    @pl.loop(inner, rows)
    def _(dr):
        relay(dr, side).wait_send()

    for dz in (second, 1, 0):

        @pl.loop(1 if isinstance(dz, int) and dz == 0 else 0, rows)
        def _(dr):
            answer(dz, dr).wait_send()


def finish_kernel(*refs):
    count = len(refs) // 2
    sems = refs[-1]
    copies = []
    for source, target in zip(refs[:count], refs[count:-1]):
        pieces = 8 if source.shape[0] > 4096 else 1
        size = source.shape[0] // pieces
        for piece in range(pieces):
            span = pl.ds(piece * size, size)
            copies.append(
                pltpu.make_async_copy(
                    source.at[span, :], target.at[span, :], sems.at[len(copies)]
                )
            )
            copies[-1].start()
    for copy in copies:
        copy.wait()


def finish(*arrays):
    vmem = pl.BlockSpec(memory_space=pltpu.VMEM)
    hbm = pl.BlockSpec(memory_space=pltpu.HBM)
    return pl.pallas_call(
        finish_kernel,
        name="finish",
        out_shape=tuple(jax.ShapeDtypeStruct(array.shape, array.dtype) for array in arrays),
        in_specs=[vmem] * len(arrays),
        out_specs=(hbm,) * len(arrays),
        scratch_shapes=[pltpu.SemaphoreType.DMA((8 + len(arrays),))],
        compiler_params=pltpu.CompilerParams(vmem_limit_bytes=16 * 1024 * 1024),
    )(*arrays)


def fetch(dp, rows, wanted, places, relayed, acc, embedding, state):
    slots = wanted.shape[0]
    devices = dp * rows
    lookups = places.shape[1] * places.shape[2]
    owned, columns = embedding.shape
    tiles = (owned // LANES, LANES)
    vmem = pl.BlockSpec(memory_space=pltpu.VMEM)
    hbm = pl.BlockSpec(memory_space=pltpu.HBM)
    table, new_state, next_rows = pl.pallas_call(
        functools.partial(fetch_kernel, dp, rows),
        name="fetch",
        out_shape=(
            jax.ShapeDtypeStruct((owned, columns), jnp.float32),
            jax.ShapeDtypeStruct(tiles, jnp.float32),
            jax.ShapeDtypeStruct((lookups, columns), jnp.bfloat16),
        ),
        in_specs=[hbm] + [vmem] * 5,
        out_specs=(vmem,) * 3,
        scratch_shapes=[
            pltpu.SMEM((slots,), jnp.int32),
            pltpu.VMEM((slots // devices, columns), jnp.float32),
            pltpu.VMEM((slots, columns), jnp.bfloat16),
            pltpu.VMEM((slots, columns), jnp.bfloat16),
            pltpu.VMEM((slots // 2, columns), jnp.bfloat16),
            pltpu.VMEM((lookups, LANES), jnp.int32),
            pltpu.VMEM((lookups, columns), jnp.float32),
            pltpu.VMEM((lookups, columns), jnp.bfloat16),
            pltpu.VMEM((lookups, columns), jnp.bfloat16),
            pltpu.VMEM(tiles, jnp.float32),
            pltpu.SemaphoreType.DMA,
            pltpu.SemaphoreType.DMA((devices,)),
            pltpu.SemaphoreType.DMA((devices,)),
            pltpu.SemaphoreType.DMA((2 * rows,)),
            pltpu.SemaphoreType.DMA((2,)),
        ],
        compiler_params=pltpu.CompilerParams(
            collective_id=1, has_side_effects=True, vmem_limit_bytes=40 * 1024 * 1024
        ),
    )(wanted, places, relayed, acc, embedding, state.reshape(tiles))
    new_embedding, new_state, next_rows = finish(table, new_state, next_rows)
    return new_embedding, new_state.reshape(owned), next_rows


def on_device(owners, offsets, gradients, embedding, adagrad_state, next_owners, next_offsets):
    dp, rows = lax.axis_size("dp"), lax.axis_size("rows")
    acc, met, places, relayed = send_gradients(
        dp, rows, owners, offsets, next_owners, next_offsets, gradients, embedding.shape[0]
    )
    wanted = met[:, 0, met.shape[2] // 2 :].reshape(-1)
    new_embedding, new_state, next_rows = fetch(
        dp, rows, wanted, places, relayed, acc, embedding, adagrad_state
    )
    return (new_embedding, new_state, next_rows)


def solution(mesh):
    in_specs = (
        P(("dp", "rows"), None),
        P(("dp", "rows")),
        P(("dp", "rows"), None),
        P(("dp", "rows"), None),
        P(("dp", "rows")),
        P(("dp", "rows"), None),
        P(("dp", "rows")),
    )
    out_specs = (P(("dp", "rows"), None), P(("dp", "rows")), P(("dp", "rows"), None))
    return jax.shard_map(
        on_device, mesh=mesh, in_specs=in_specs, out_specs=out_specs, check_vma=False
    )
```

```python
import functools

import jax
import jax.numpy as jnp
from jax import lax
from jax.experimental import pallas as pl
from jax.experimental.pallas import tpu as pltpu
from jax.sharding import PartitionSpec as P

LANES = 128
SUB = 16
BASE = 256
MESH = pl.DeviceIdType.MESH


def flip(value, step, size):
    bit, result = 1, value
    while bit < size:
        own = lax.rem(lax.div(value, bit), 2)
        if isinstance(step, int):
            if step // bit % 2:
                result = result + bit * (1 - 2 * own)
        else:
            other = lax.rem(lax.div(step, bit), 2)
            result = result + bit * other * (1 - 2 * own)
        bit *= 2
    return result


def is_inner(dp):
    return lax.rem(lax.div(lax.axis_index("dp") + 1, 2), 2)


def peer(dp, rows, dz, dr):
    z, r = lax.axis_index("dp"), lax.axis_index("rows")
    return (flip(z, dz, dp), flip(r, dr, rows))


def greet(dp, rows):
    barrier = pltpu.get_barrier_semaphore()
    for i in range(1, dp * rows):
        pl.semaphore_signal(
            barrier, inc=1, device_id=peer(dp, rows, i // rows, i % rows), device_id_type=MESH
        )


def gathered(dp, rows):
    pl.semaphore_wait(pltpu.get_barrier_semaphore(), dp * rows - 1)


def selectors(names, count):
    shape = (SUB, names.shape[1])
    low = lax.broadcasted_iota(jnp.int32, shape, 0) == names % SUB
    ones = jnp.where(low, 1.0, 0.0).astype(jnp.bfloat16)
    high = jnp.broadcast_to((names // SUB).astype(jnp.float32), shape)

    def pick(start):
        shifted = (high - start).astype(jnp.bfloat16)
        zero = jnp.zeros(shape, jnp.bfloat16)
        return jnp.concatenate(
            [jnp.where(shifted == jnp.bfloat16(k), ones, zero) for k in range(count // SUB)], axis=0
        )

    return pick


def route(names, values, me, devices, capacity):
    blocks = names.shape[0]
    columns = names.shape[1]
    relative = jnp.bitwise_xor(names, me)
    index = lax.broadcasted_iota(jnp.int32, (devices, columns), 0)
    hits = [jnp.where(index == relative[b : b + 1, :], 1.0, 0.0) for b in range(blocks)]
    before = jnp.where(
        lax.broadcasted_iota(jnp.int32, (columns, columns), 0)
        < lax.broadcasted_iota(jnp.int32, (columns, columns), 1),
        1.0,
        0.0,
    ).astype(jnp.bfloat16)
    one_hot = [hit.astype(jnp.bfloat16) for hit in hits]
    ahead = jnp.dot(
        jnp.concatenate(one_hot, axis=0), before, preferred_element_type=jnp.float32
    )
    seen = jnp.zeros((devices, 1), jnp.float32)
    slots = []
    for b in range(blocks):
        within = ahead[b * devices : (b + 1) * devices, :] + seen
        slots.append(jnp.sum(hits[b] * within, axis=0, keepdims=True))
        seen = seen + jnp.sum(hits[b], axis=1, keepdims=True)
    slots = jnp.concatenate(slots, axis=0).astype(jnp.int32)
    high = (values // BASE).astype(jnp.float32)
    low = (values % BASE).astype(jnp.float32)
    place = lax.broadcasted_iota(jnp.int32, (capacity, columns), 0)
    marked = []
    for b in range(blocks):
        taken = place == slots[b : b + 1, :]
        marked.append(
            jnp.concatenate(
                [jnp.where(taken, high[b : b + 1, :], 0.0), jnp.where(taken, low[b : b + 1, :], 0.0)],
                axis=0,
            ).astype(jnp.bfloat16)
        )
    table = lax.dot_general(
        jnp.concatenate(one_hot, axis=1),
        jnp.concatenate(marked, axis=1),
        (((1,), (1,)), ((), ())),
        preferred_element_type=jnp.float32,
    )
    table = (table[:, :capacity] * BASE + table[:, capacity:]).astype(jnp.int32)
    return relative * capacity + slots, table


def send_kernel(
    dp, rows,
    index_ref, gradients_ref,
    acc_ref, met_ref, places_ref, relayed_ref,
    flat, meta_ref, outgoing, incoming, raw, relay_out,
    meta_send, meta_recv, data_send, data_recv, relay_send, raw_sems,
):
    devices = dp * rows
    slots = outgoing.shape[0]
    capacity = slots // devices
    columns = gradients_ref.shape[1]
    half = acc_ref.shape[0]
    group = 2 if capacity == LANES else 1
    depth = group * capacity

    greet(dp, rows)

    me = lax.axis_index("dp") * rows + lax.axis_index("rows")
    place, table = route(index_ref[0], index_ref[1], me, devices, capacity)
    next_place, next_table = route(index_ref[2], index_ref[3], me, devices, capacity)
    places_ref[0] = place
    places_ref[1] = next_place
    flat[...] = jnp.concatenate([table, next_table], axis=1)
    for i in range(devices):
        meta_ref[i] = flat[i : i + 1, :]

    inner = is_inner(dp)
    plane = rows * capacity
    made = min(512, plane)

    def builder(place):
        return selectors(
            jnp.concatenate([place[b : b + 1, :] for b in range(place.shape[0])], axis=1), made
        )

    def build(pick, source, target, dz, base):
        @pl.loop(0, plane // made)
        def _(step):
            first = dz * plane + step * made
            target[pl.ds(pl.multiple_of(first - base, made), made), :] = jnp.dot(
                pick(jnp.float32(first // SUB) if isinstance(first, int)
                     else (first // SUB).astype(jnp.float32)),
                source[...],
                preferred_element_type=jnp.float32,
            ).astype(jnp.bfloat16)

    def span_of(i):
        return pl.ds(pl.multiple_of(i * capacity, capacity), capacity)

    def send_meta(dz, dr):
        i = dz * rows + dr
        return pltpu.make_async_remote_copy(
            src_ref=meta_ref.at[i], dst_ref=met_ref.at[i],
            send_sem=meta_send.at[i], recv_sem=meta_recv.at[i],
            device_id=peer(dp, rows, dz, dr), device_id_type=MESH,
        )

    def send_data(dz, dr):
        i = dz * rows + dr
        return pltpu.make_async_remote_copy(
            src_ref=outgoing.at[span_of(i), :], dst_ref=incoming.at[span_of(i), :],
            send_sem=data_send.at[i], recv_sem=data_recv.at[i],
            device_id=peer(dp, rows, dz, dr), device_id_type=MESH,
        )

    def relay_data(dz, dr):
        i = dz * rows + dr
        k = i - 2 * rows
        return pltpu.make_async_remote_copy(
            src_ref=relay_out.at[span_of(k), :], dst_ref=incoming.at[span_of(i), :],
            send_sem=relay_send.at[k], recv_sem=data_recv.at[i],
            device_id=peer(dp, rows, dz - 2, dr), device_id_type=MESH,
        )

    def send_raw():
        to = peer(dp, rows, 2, 0)
        return (
            pltpu.make_async_remote_copy(
                src_ref=places_ref, dst_ref=relayed_ref,
                send_sem=raw_sems.at[0], recv_sem=raw_sems.at[1],
                device_id=to, device_id_type=MESH,
            ),
            pltpu.make_async_remote_copy(
                src_ref=gradients_ref, dst_ref=raw,
                send_sem=raw_sems.at[2], recv_sem=raw_sems.at[3],
                device_id=to, device_id_type=MESH,
            ),
        )

    pick = builder(place)
    build(pick, gradients_ref, outgoing, 1, 0)
    gathered(dp, rows)

    @pl.when(inner == 0)
    def _():
        for copy in send_raw():
            copy.start()

    for dz in (2, 1, 3, 0):
        for dr in range(0 if dz else 1, rows):
            send_meta(dz, dr).start()

    def send_plane(dz):
        for dr in range(0 if dz else 1, rows):
            send_data(dz, dr).start()

    send_plane(1)
    build(pick, gradients_ref, outgoing, 0, 0)
    send_plane(0)

    @pl.when(inner == 1)
    def _():
        for dz in (2, 3):
            build(pick, gradients_ref, outgoing, dz, 0)
            send_plane(dz)

    @pl.loop(0, half // LANES)
    def _(step):
        acc_ref[pl.ds(pl.multiple_of(step * LANES, LANES), LANES), :] = jnp.zeros(
            (LANES, acc_ref.shape[1]), jnp.float32
        )

    met_ref[0] = meta_ref[0]
    incoming[0:capacity, :] = outgoing[0:capacity, :]

    chunk = min(4096, half)

    def accumulate(tile):
        met = [met_ref[tile * group + k][:, :capacity] for k in range(group)]
        parts = []
        for k in range(group):
            side = jnp.broadcast_to((met[k] // half).astype(jnp.float32), (columns, capacity)).T
            start = pl.multiple_of((tile * group + k) * capacity, capacity)
            block = incoming[pl.ds(start, capacity), :].astype(jnp.float32)
            parts.append(
                jnp.concatenate(
                    [jnp.where(side > 0.5, 0.0, block), jnp.where(side > 0.5, block, 0.0)], axis=1
                ).astype(jnp.bfloat16)
            )
        wide = jnp.concatenate(parts, axis=0) if group > 1 else parts[0]
        names = (jnp.concatenate(met, axis=1) if group > 1 else met[0]) % half
        pick_rows = selectors(names, chunk)

        @pl.loop(0, half // chunk)
        def _(step):
            span = pl.ds(pl.multiple_of(step * chunk, chunk), chunk)
            acc_ref[span, :] += jnp.dot(
                pick_rows((step * (chunk // SUB)).astype(jnp.float32)),
                wide,
                preferred_element_type=jnp.float32,
            )

    per_plane = rows // group

    def take_plane(dz):
        @pl.loop(0, per_plane)
        def _(step):
            for k in range(group):
                dr = step * group + k

                def arrive_meta():
                    send_meta(dz, dr).wait_recv()

                def arrive():
                    send_data(dz, dr).wait_recv()

                if dz == 0:
                    pl.when(dr > 0)(arrive_meta)
                    pl.when(dr > 0)(arrive)
                elif dz == 2:
                    arrive_meta()
                    pl.when(dr + (1 - inner) > 0)(arrive)
                else:
                    arrive_meta()
                    arrive()
            accumulate(dz * per_plane + step)

    take_plane(0)

    @pl.when(inner == 1)
    def _():
        for copy in send_raw():
            copy.wait_recv()
        relay_pick = builder(relayed_ref[0])
        for dz in (3, 2):
            build(relay_pick, raw, relay_out, dz, 2 * plane)
            for dr in range(0 if dz == 3 else 1, rows):
                relay_data(dz, dr).start()
        incoming[2 * plane : 2 * plane + capacity, :] = relay_out[0:capacity, :]

    take_plane(1)
    take_plane(2)
    take_plane(3)

    for dz in range(dp):

        @pl.loop(0 if dz else 1, rows)
        def _(dr):
            send_meta(dz, dr).wait_send()
            if dz < 2:
                send_data(dz, dr).wait_send()

    @pl.when(inner == 1)
    def _():
        for dz in (2, 3):

            @pl.loop(0, rows)
            def _(dr):
                send_data(dz, dr).wait_send()

            @pl.loop(0 if dz == 3 else 1, rows)
            def _(dr):
                relay_data(dz, dr).wait_send()

    @pl.when(inner == 0)
    def _():
        for copy in send_raw():
            copy.wait_send()


def send_gradients(dp, rows, owners, offsets, next_owners, next_offsets, gradients, owned):
    devices = dp * rows
    lookups, columns = gradients.shape
    capacity = max(2, 4 * lookups // devices)
    slots = devices * capacity
    vmem = pl.BlockSpec(memory_space=pltpu.VMEM)
    tiles = (lookups // LANES, LANES)
    return pl.pallas_call(
        functools.partial(send_kernel, dp, rows),
        name="send_gradients",
        out_shape=(
            jax.ShapeDtypeStruct((owned // 2, 2 * columns), jnp.float32),
            jax.ShapeDtypeStruct((devices, 1, 2 * capacity), jnp.int32),
            jax.ShapeDtypeStruct((2,) + tiles, jnp.int32),
            jax.ShapeDtypeStruct((2,) + tiles, jnp.int32),
        ),
        in_specs=[vmem] * 2,
        out_specs=(vmem,) * 4,
        scratch_shapes=[
            pltpu.VMEM((devices, 2 * capacity), jnp.int32),
            pltpu.VMEM((devices, 1, 2 * capacity), jnp.int32),
            pltpu.VMEM((slots, columns), jnp.bfloat16),
            pltpu.VMEM((slots, columns), jnp.bfloat16),
            pltpu.VMEM((lookups, columns), jnp.bfloat16),
            pltpu.VMEM((2 * rows * capacity, columns), jnp.bfloat16),
        ]
        + [pltpu.SemaphoreType.DMA((devices,))] * 4
        + [pltpu.SemaphoreType.DMA((2 * rows,)), pltpu.SemaphoreType.DMA((4,))],
        compiler_params=pltpu.CompilerParams(
            collective_id=0, has_side_effects=True, vmem_limit_bytes=40 * 1024 * 1024
        ),
        cost_estimate=pl.CostEstimate(
            flops=400 * slots * owned * columns, bytes_accessed=owned * columns * 4, transcendentals=0
        ),
    )(
        jnp.stack([part.reshape(tiles) for part in (owners, offsets, next_owners, next_offsets)]),
        gradients,
    )


def split(x):
    high = x.astype(jnp.bfloat16)
    return high, (x - high.astype(jnp.float32)).astype(jnp.bfloat16)


def update(acc_ref, embedding_ref, state_ref, new_state_ref, rate_ref, table):
    half = acc_ref.shape[0]
    tiles = half // LANES
    eye = lax.broadcasted_iota(jnp.int32, (LANES, LANES), 0) == lax.broadcasted_iota(
        jnp.int32, (LANES, LANES), 1
    )
    same = jnp.where(eye, 1.0, 0.0).astype(jnp.bfloat16)
    ones = jnp.ones((2 * LANES, LANES), jnp.bfloat16)
    sides = table.shape[0] // half

    batch = min(16, tiles)

    for side in range(sides):

        @pl.loop(0, tiles // batch)
        def _(step):
            low = pl.ds(pl.multiple_of(step * batch * LANES, batch * LANES), batch * LANES)
            grad_sum = acc_ref[low, side * LANES : (side + 1) * LANES]
            square = jnp.concatenate(split(grad_sum * grad_sum), axis=1)
            sums = jnp.dot(square, ones, preferred_element_type=jnp.float32)
            means = [
                jnp.sum(
                    jnp.where(eye, sums[k * LANES : (k + 1) * LANES, :], 0.0), axis=0, keepdims=True
                )
                for k in range(batch)
            ]
            first = pl.multiple_of(side * tiles + step * batch, batch)
            rate_ref[pl.ds(first, batch), :] = jnp.concatenate(means, axis=0)

    state = state_ref[...] + rate_ref[...] * (1.0 / LANES)
    new_state_ref[...] = state
    rate_ref[...] = 0.5 * lax.rsqrt(state)

    for side in range(sides):

        @pl.loop(0, tiles // batch)
        def _(step):
            first = pl.multiple_of(side * tiles + step * batch, batch)
            rows = batch * LANES
            span = pl.ds(pl.multiple_of(first * LANES, rows), rows)
            low = pl.ds(pl.multiple_of(step * rows, rows), rows)
            parts = split(rate_ref[pl.ds(first, batch), :])
            diagonal = jnp.concatenate(
                [
                    jnp.concatenate([same * part[k : k + 1, :] for part in parts], axis=1)
                    for k in range(batch)
                ],
                axis=0,
            )
            rate = jnp.dot(diagonal, ones, preferred_element_type=jnp.float32)
            grad_sum = acc_ref[low, side * LANES : (side + 1) * LANES]
            table[span, :] = embedding_ref[span, :] - grad_sum * rate


def fetch_kernel(
    dp, rows,
    wanted_hbm, places_ref, relayed_ref, acc_ref, embedding_ref, state_ref,
    table, new_state_ref, next_ref,
    wanted_ref, picked, outgoing, incoming, relay_in, place, total, partial, summed, rate_ref,
    wanted_sem, data_send, data_recv, relay_recv, raw_sems,
):
    devices = dp * rows
    slots = outgoing.shape[0]
    capacity = slots // devices
    group = 2 if capacity == LANES else 1
    depth = group * capacity

    greet(dp, rows)
    load = pltpu.make_async_copy(wanted_hbm, wanted_ref, wanted_sem)
    load.start()
    update(acc_ref, embedding_ref, state_ref, new_state_ref, rate_ref, table)
    load.wait()

    inner = is_inner(dp)
    plane = rows * capacity
    z, r = lax.axis_index("dp"), lax.axis_index("rows")

    def span_of(i):
        return pl.ds(pl.multiple_of(i * capacity, capacity), capacity)

    def answer(dz, dr):
        i = dz * rows + dr
        return pltpu.make_async_remote_copy(
            src_ref=outgoing.at[span_of(i), :], dst_ref=incoming.at[span_of(i), :],
            send_sem=data_send.at[i], recv_sem=data_recv.at[i],
            device_id=peer(dp, rows, dz, dr), device_id_type=MESH,
        )

    def relay(dr, side):
        i = (3 - inner) * rows + dr
        k = side * rows + dr
        return pltpu.make_async_remote_copy(
            src_ref=outgoing.at[span_of(i), :], dst_ref=relay_in.at[span_of(k), :],
            send_sem=data_send.at[i], recv_sem=relay_recv.at[k],
            device_id=(z + (1 - inner) * (1 - 2 * lax.rem(z, 2)), flip(r, dr, rows)),
            device_id_type=MESH,
        )

    def send_raw():
        return pltpu.make_async_remote_copy(
            src_ref=summed, dst_ref=partial, send_sem=raw_sems.at[0], recv_sem=raw_sems.at[1],
            device_id=peer(dp, rows, 2, 0), device_id_type=MESH,
        )

    def gather(i):
        start = pl.multiple_of(i * capacity, capacity)
        for k in range(capacity):
            picked[pl.ds(k, 1), :] = table[pl.ds(wanted_ref[start + k], 1), :]
        outgoing[pl.ds(start, capacity), :] = picked[...].astype(jnp.bfloat16)

    first, second = 3 - inner, 2 + inner
    gather(first * rows)
    gathered(dp, rows)
    side = 1 - inner

    for dr in range(1, rows):
        gather(first * rows + dr)
        if dr == 1:
            pl.when(inner == 0)(lambda: relay(0, side).start())
        else:
            relay(dr - 1, side).start()
    relay(rows - 1, side).start()

    for dz in (second, 1, 0):

        @pl.loop(0, rows)
        def _(dr):
            gather(dz * rows + dr)

        for dr in range(1 if isinstance(dz, int) and dz == 0 else 0, rows):
            answer(dz, dr).start()

    lookups = total.shape[0]
    per_plane = rows // group

    def turn(source):
        for b in range(source.shape[0]):
            row = source[b : b + 1, :].astype(jnp.float32)
            place[b * LANES : (b + 1) * LANES, :] = jnp.broadcast_to(row, (LANES, LANES)).T.astype(
                jnp.int32
            )
        total[...] = jnp.zeros(total.shape, jnp.float32)

    def put(base, blocks, start):
        lane = lax.broadcasted_iota(jnp.int32, (lookups, capacity), 1)
        chosen = jnp.concatenate(
            [
                jnp.where(place[:, :capacity] == lane + (base + start + k * capacity), 1.0, 0.0)
                for k in range(group)
            ],
            axis=1,
        ).astype(jnp.bfloat16)
        total[...] += jnp.dot(
            chosen, blocks[pl.ds(start, depth), :], preferred_element_type=jnp.float32
        )

    @pl.when(inner == 1)
    def _():
        relay_in[0:capacity, :] = outgoing[2 * plane : 2 * plane + capacity, :]
        turn(relayed_ref[1])
        for half in range(2):

            @pl.loop(0, per_plane)
            def _(step):
                for k in range(group):
                    dr = step * group + k

                    def arrive():
                        relay(dr, half).wait_recv()

                    if half == 0:
                        pl.when(dr > 0)(arrive)
                    else:
                        arrive()
                start = half * plane + step * depth
                put(2 * plane, relay_in, pl.multiple_of(start, depth))

        summed[...] = total[...].astype(jnp.bfloat16)

    turn(places_ref[1])

    @pl.when(inner == 1)
    def _():
        send_raw().start()

    incoming[0:capacity, :] = outgoing[0:capacity, :]

    def take_plane(dz):
        @pl.loop(0, per_plane)
        def _(step):
            for k in range(group):
                dr = step * group + k

                def arrive():
                    answer(dz, dr).wait_recv()

                if dz == 0:
                    pl.when(dr > 0)(arrive)
                else:
                    arrive()
            put(0, incoming, pl.multiple_of(dz * plane + step * depth, depth))

    take_plane(0)
    take_plane(1)

    @pl.when(inner == 1)
    def _():
        take_plane(2)
        take_plane(3)
        next_ref[...] = total[...].astype(jnp.bfloat16)
        send_raw().wait_send()

    @pl.when(inner == 0)
    def _():
        send_raw().wait_recv()
        next_ref[...] = (total[...] + partial[...].astype(jnp.float32)).astype(jnp.bfloat16)

    @pl.loop(inner, rows)
    def _(dr):
        relay(dr, side).wait_send()

    for dz in (second, 1, 0):

        @pl.loop(1 if isinstance(dz, int) and dz == 0 else 0, rows)
        def _(dr):
            answer(dz, dr).wait_send()


def finish_kernel(*refs):
    count = len(refs) // 2
    sems = refs[-1]
    copies = []
    for source, target in zip(refs[:count], refs[count:-1]):
        pieces = 8 if source.shape[0] > 4096 else 1
        size = source.shape[0] // pieces
        for piece in range(pieces):
            span = pl.ds(piece * size, size)
            copies.append(
                pltpu.make_async_copy(
                    source.at[span, :], target.at[span, :], sems.at[len(copies)]
                )
            )
            copies[-1].start()
    for copy in copies:
        copy.wait()


def finish(*arrays):
    vmem = pl.BlockSpec(memory_space=pltpu.VMEM)
    hbm = pl.BlockSpec(memory_space=pltpu.HBM)
    return pl.pallas_call(
        finish_kernel,
        name="finish",
        out_shape=tuple(jax.ShapeDtypeStruct(array.shape, array.dtype) for array in arrays),
        in_specs=[vmem] * len(arrays),
        out_specs=(hbm,) * len(arrays),
        scratch_shapes=[pltpu.SemaphoreType.DMA((8 + len(arrays),))],
        compiler_params=pltpu.CompilerParams(vmem_limit_bytes=16 * 1024 * 1024),
    )(*arrays)


def fetch(dp, rows, wanted, places, relayed, acc, embedding, state):
    slots = wanted.shape[0]
    devices = dp * rows
    lookups = places.shape[1] * places.shape[2]
    owned, columns = embedding.shape
    tiles = (owned // LANES, LANES)
    vmem = pl.BlockSpec(memory_space=pltpu.VMEM)
    hbm = pl.BlockSpec(memory_space=pltpu.HBM)
    table, new_state, next_rows = pl.pallas_call(
        functools.partial(fetch_kernel, dp, rows),
        name="fetch",
        out_shape=(
            jax.ShapeDtypeStruct((owned, columns), jnp.float32),
            jax.ShapeDtypeStruct(tiles, jnp.float32),
            jax.ShapeDtypeStruct((lookups, columns), jnp.bfloat16),
        ),
        in_specs=[hbm] + [vmem] * 5,
        out_specs=(vmem,) * 3,
        scratch_shapes=[
            pltpu.SMEM((slots,), jnp.int32),
            pltpu.VMEM((slots // devices, columns), jnp.float32),
            pltpu.VMEM((slots, columns), jnp.bfloat16),
            pltpu.VMEM((slots, columns), jnp.bfloat16),
            pltpu.VMEM((slots // 2, columns), jnp.bfloat16),
            pltpu.VMEM((lookups, LANES), jnp.int32),
            pltpu.VMEM((lookups, columns), jnp.float32),
            pltpu.VMEM((lookups, columns), jnp.bfloat16),
            pltpu.VMEM((lookups, columns), jnp.bfloat16),
            pltpu.VMEM(tiles, jnp.float32),
            pltpu.SemaphoreType.DMA,
            pltpu.SemaphoreType.DMA((devices,)),
            pltpu.SemaphoreType.DMA((devices,)),
            pltpu.SemaphoreType.DMA((2 * rows,)),
            pltpu.SemaphoreType.DMA((2,)),
        ],
        compiler_params=pltpu.CompilerParams(
            collective_id=1, has_side_effects=True, vmem_limit_bytes=40 * 1024 * 1024
        ),
    )(wanted, places, relayed, acc, embedding, state.reshape(tiles))
    new_embedding, new_state, next_rows = finish(table, new_state, next_rows)
    return new_embedding, new_state.reshape(owned), next_rows


def on_device(owners, offsets, gradients, embedding, adagrad_state, next_owners, next_offsets):
    dp, rows = lax.axis_size("dp"), lax.axis_size("rows")
    acc, met, places, relayed = send_gradients(
        dp, rows, owners, offsets, next_owners, next_offsets, gradients, embedding.shape[0]
    )
    wanted = met[:, 0, met.shape[2] // 2 :].reshape(-1)
    new_embedding, new_state, next_rows = fetch(
        dp, rows, wanted, places, relayed, acc, embedding, adagrad_state
    )
    return (new_embedding, new_state, next_rows)


def solution(mesh):
    in_specs = (
        P(("dp", "rows"), None),
        P(("dp", "rows")),
        P(("dp", "rows"), None),
        P(("dp", "rows"), None),
        P(("dp", "rows")),
        P(("dp", "rows"), None),
        P(("dp", "rows")),
    )
    out_specs = (P(("dp", "rows"), None), P(("dp", "rows")), P(("dp", "rows"), None))
    return jax.shard_map(
        on_device, mesh=mesh, in_specs=in_specs, out_specs=out_specs, check_vma=False
    )
```

```python
import functools

import jax
import jax.numpy as jnp
from jax import lax
from jax.experimental import pallas as pl
from jax.experimental.pallas import tpu as pltpu
from jax.sharding import PartitionSpec as P

LANES = 128
SUB = 16
BASE = 256
MESH = pl.DeviceIdType.MESH


def flip(value, step, size):
    bit, result = 1, value
    while bit < size:
        own = lax.rem(lax.div(value, bit), 2)
        if isinstance(step, int):
            if step // bit % 2:
                result = result + bit * (1 - 2 * own)
        else:
            other = lax.rem(lax.div(step, bit), 2)
            result = result + bit * other * (1 - 2 * own)
        bit *= 2
    return result


def is_inner(dp):
    return lax.rem(lax.div(lax.axis_index("dp") + 1, 2), 2)


def peer(dp, rows, dz, dr):
    z, r = lax.axis_index("dp"), lax.axis_index("rows")
    return (flip(z, dz, dp), flip(r, dr, rows))


def greet(dp, rows):
    barrier = pltpu.get_barrier_semaphore()
    for i in range(1, dp * rows):
        pl.semaphore_signal(
            barrier, inc=1, device_id=peer(dp, rows, i // rows, i % rows), device_id_type=MESH
        )


def gathered(dp, rows):
    pl.semaphore_wait(pltpu.get_barrier_semaphore(), dp * rows - 1)


def selectors(names, count):
    shape = (SUB, names.shape[1])
    low = lax.broadcasted_iota(jnp.int32, shape, 0) == names % SUB
    ones = jnp.where(low, 1.0, 0.0).astype(jnp.bfloat16)
    high = jnp.broadcast_to((names // SUB).astype(jnp.float32), shape)

    def pick(start):
        shifted = (high - start).astype(jnp.bfloat16)
        zero = jnp.zeros(shape, jnp.bfloat16)
        return jnp.concatenate(
            [jnp.where(shifted == jnp.bfloat16(k), ones, zero) for k in range(count // SUB)], axis=0
        )

    return pick


def route(names, values, me, devices, capacity):
    blocks = names.shape[0]
    columns = names.shape[1]
    relative = jnp.bitwise_xor(names, me)
    index = lax.broadcasted_iota(jnp.int32, (devices, columns), 0)
    hits = [jnp.where(index == relative[b : b + 1, :], 1.0, 0.0) for b in range(blocks)]
    before = jnp.where(
        lax.broadcasted_iota(jnp.int32, (columns, columns), 0)
        < lax.broadcasted_iota(jnp.int32, (columns, columns), 1),
        1.0,
        0.0,
    ).astype(jnp.bfloat16)
    one_hot = [hit.astype(jnp.bfloat16) for hit in hits]
    ahead = jnp.dot(
        jnp.concatenate(one_hot, axis=0), before, preferred_element_type=jnp.float32
    )
    seen = jnp.zeros((devices, 1), jnp.float32)
    slots = []
    for b in range(blocks):
        within = ahead[b * devices : (b + 1) * devices, :] + seen
        slots.append(jnp.sum(hits[b] * within, axis=0, keepdims=True))
        seen = seen + jnp.sum(hits[b], axis=1, keepdims=True)
    slots = jnp.concatenate(slots, axis=0).astype(jnp.int32)
    high = (values // BASE).astype(jnp.float32)
    low = (values % BASE).astype(jnp.float32)
    place = lax.broadcasted_iota(jnp.int32, (capacity, columns), 0)
    marked = []
    for b in range(blocks):
        taken = place == slots[b : b + 1, :]
        marked.append(
            jnp.concatenate(
                [jnp.where(taken, high[b : b + 1, :], 0.0), jnp.where(taken, low[b : b + 1, :], 0.0)],
                axis=0,
            ).astype(jnp.bfloat16)
        )
    table = lax.dot_general(
        jnp.concatenate(one_hot, axis=1),
        jnp.concatenate(marked, axis=1),
        (((1,), (1,)), ((), ())),
        preferred_element_type=jnp.float32,
    )
    table = (table[:, :capacity] * BASE + table[:, capacity:]).astype(jnp.int32)
    return relative * capacity + slots, table


def send_kernel(
    dp, rows,
    index_ref, gradients_ref,
    acc_ref, met_ref, places_ref, relayed_ref,
    flat, meta_ref, outgoing, incoming, raw, relay_out,
    meta_send, meta_recv, data_send, data_recv, relay_send, raw_sems,
):
    devices = dp * rows
    slots = outgoing.shape[0]
    capacity = slots // devices
    columns = gradients_ref.shape[1]
    half = acc_ref.shape[0]
    group = 2 if capacity == LANES else 1
    depth = group * capacity

    greet(dp, rows)

    me = lax.axis_index("dp") * rows + lax.axis_index("rows")
    place, table = route(index_ref[0], index_ref[1], me, devices, capacity)
    next_place, next_table = route(index_ref[2], index_ref[3], me, devices, capacity)
    places_ref[0] = place
    places_ref[1] = next_place
    flat[...] = jnp.concatenate([table, next_table], axis=1)
    for i in range(devices):
        meta_ref[i] = flat[i : i + 1, :]

    inner = is_inner(dp)
    plane = rows * capacity
    made = min(512, plane)

    def builder(place):
        return selectors(
            jnp.concatenate([place[b : b + 1, :] for b in range(place.shape[0])], axis=1), made
        )

    def build(pick, source, target, dz, base):
        @pl.loop(0, plane // made)
        def _(step):
            first = dz * plane + step * made
            target[pl.ds(pl.multiple_of(first - base, made), made), :] = jnp.dot(
                pick(jnp.float32(first // SUB) if isinstance(first, int)
                     else (first // SUB).astype(jnp.float32)),
                source[...],
                preferred_element_type=jnp.float32,
            ).astype(jnp.bfloat16)

    def span_of(i):
        return pl.ds(pl.multiple_of(i * capacity, capacity), capacity)

    def send_meta(dz, dr):
        i = dz * rows + dr
        return pltpu.make_async_remote_copy(
            src_ref=meta_ref.at[i], dst_ref=met_ref.at[i],
            send_sem=meta_send.at[i], recv_sem=meta_recv.at[i],
            device_id=peer(dp, rows, dz, dr), device_id_type=MESH,
        )

    def send_data(dz, dr):
        i = dz * rows + dr
        return pltpu.make_async_remote_copy(
            src_ref=outgoing.at[span_of(i), :], dst_ref=incoming.at[span_of(i), :],
            send_sem=data_send.at[i], recv_sem=data_recv.at[i],
            device_id=peer(dp, rows, dz, dr), device_id_type=MESH,
        )

    def relay_data(dz, dr):
        i = dz * rows + dr
        k = i - 2 * rows
        return pltpu.make_async_remote_copy(
            src_ref=relay_out.at[span_of(k), :], dst_ref=incoming.at[span_of(i), :],
            send_sem=relay_send.at[k], recv_sem=data_recv.at[i],
            device_id=peer(dp, rows, dz - 2, dr), device_id_type=MESH,
        )

    def send_raw():
        to = peer(dp, rows, 2, 0)
        return (
            pltpu.make_async_remote_copy(
                src_ref=places_ref, dst_ref=relayed_ref,
                send_sem=raw_sems.at[0], recv_sem=raw_sems.at[1],
                device_id=to, device_id_type=MESH,
            ),
            pltpu.make_async_remote_copy(
                src_ref=gradients_ref, dst_ref=raw,
                send_sem=raw_sems.at[2], recv_sem=raw_sems.at[3],
                device_id=to, device_id_type=MESH,
            ),
        )

    pick = builder(place)
    build(pick, gradients_ref, outgoing, 1, 0)
    gathered(dp, rows)

    @pl.when(inner == 0)
    def _():
        for copy in send_raw():
            copy.start()

    for dz in (2, 1, 3, 0):
        for dr in range(0 if dz else 1, rows):
            send_meta(dz, dr).start()

    def send_plane(dz):
        for dr in range(0 if dz else 1, rows):
            send_data(dz, dr).start()

    send_plane(1)
    build(pick, gradients_ref, outgoing, 0, 0)
    send_plane(0)

    @pl.when(inner == 1)
    def _():
        for dz in (2, 3):
            build(pick, gradients_ref, outgoing, dz, 0)
            send_plane(dz)

    @pl.loop(0, half // LANES)
    def _(step):
        acc_ref[pl.ds(pl.multiple_of(step * LANES, LANES), LANES), :] = jnp.zeros(
            (LANES, acc_ref.shape[1]), jnp.float32
        )

    met_ref[0] = meta_ref[0]
    incoming[0:capacity, :] = outgoing[0:capacity, :]

    chunk = min(4096, half)

    def accumulate(tile):
        met = [met_ref[tile * group + k][:, :capacity] for k in range(group)]
        parts = []
        for k in range(group):
            side = jnp.broadcast_to((met[k] // half).astype(jnp.float32), (columns, capacity)).T
            start = pl.multiple_of((tile * group + k) * capacity, capacity)
            block = incoming[pl.ds(start, capacity), :].astype(jnp.float32)
            parts.append(
                jnp.concatenate(
                    [jnp.where(side > 0.5, 0.0, block), jnp.where(side > 0.5, block, 0.0)], axis=1
                ).astype(jnp.bfloat16)
            )
        wide = jnp.concatenate(parts, axis=0) if group > 1 else parts[0]
        names = (jnp.concatenate(met, axis=1) if group > 1 else met[0]) % half
        pick_rows = selectors(names, chunk)

        @pl.loop(0, half // chunk)
        def _(step):
            span = pl.ds(pl.multiple_of(step * chunk, chunk), chunk)
            acc_ref[span, :] += jnp.dot(
                pick_rows((step * (chunk // SUB)).astype(jnp.float32)),
                wide,
                preferred_element_type=jnp.float32,
            )

    per_plane = rows // group

    def take_plane(dz):
        @pl.loop(0, per_plane)
        def _(step):
            for k in range(group):
                dr = step * group + k

                def arrive_meta():
                    send_meta(dz, dr).wait_recv()

                def arrive():
                    send_data(dz, dr).wait_recv()

                if dz == 0:
                    pl.when(dr > 0)(arrive_meta)
                    pl.when(dr > 0)(arrive)
                elif dz == 2:
                    arrive_meta()
                    pl.when(dr + (1 - inner) > 0)(arrive)
                else:
                    arrive_meta()
                    arrive()
            accumulate(dz * per_plane + step)

    take_plane(0)

    @pl.when(inner == 1)
    def _():
        for copy in send_raw():
            copy.wait_recv()
        relay_pick = builder(relayed_ref[0])
        for dz in (3, 2):
            build(relay_pick, raw, relay_out, dz, 2 * plane)
            for dr in range(0 if dz == 3 else 1, rows):
                relay_data(dz, dr).start()
        incoming[2 * plane : 2 * plane + capacity, :] = relay_out[0:capacity, :]

    take_plane(1)
    take_plane(2)
    take_plane(3)

    for dz in range(dp):

        @pl.loop(0 if dz else 1, rows)
        def _(dr):
            send_meta(dz, dr).wait_send()
            if dz < 2:
                send_data(dz, dr).wait_send()

    @pl.when(inner == 1)
    def _():
        for dz in (2, 3):

            @pl.loop(0, rows)
            def _(dr):
                send_data(dz, dr).wait_send()

            @pl.loop(0 if dz == 3 else 1, rows)
            def _(dr):
                relay_data(dz, dr).wait_send()

    @pl.when(inner == 0)
    def _():
        for copy in send_raw():
            copy.wait_send()


def send_gradients(dp, rows, owners, offsets, next_owners, next_offsets, gradients, owned):
    devices = dp * rows
    lookups, columns = gradients.shape
    capacity = max(2, 4 * lookups // devices)
    slots = devices * capacity
    vmem = pl.BlockSpec(memory_space=pltpu.VMEM)
    tiles = (lookups // LANES, LANES)
    return pl.pallas_call(
        functools.partial(send_kernel, dp, rows),
        name="send_gradients",
        out_shape=(
            jax.ShapeDtypeStruct((owned // 2, 2 * columns), jnp.float32),
            jax.ShapeDtypeStruct((devices, 1, 2 * capacity), jnp.int32),
            jax.ShapeDtypeStruct((2,) + tiles, jnp.int32),
            jax.ShapeDtypeStruct((2,) + tiles, jnp.int32),
        ),
        in_specs=[vmem] * 2,
        out_specs=(vmem,) * 4,
        scratch_shapes=[
            pltpu.VMEM((devices, 2 * capacity), jnp.int32),
            pltpu.VMEM((devices, 1, 2 * capacity), jnp.int32),
            pltpu.VMEM((slots, columns), jnp.bfloat16),
            pltpu.VMEM((slots, columns), jnp.bfloat16),
            pltpu.VMEM((lookups, columns), jnp.bfloat16),
            pltpu.VMEM((2 * rows * capacity, columns), jnp.bfloat16),
        ]
        + [pltpu.SemaphoreType.DMA((devices,))] * 4
        + [pltpu.SemaphoreType.DMA((2 * rows,)), pltpu.SemaphoreType.DMA((4,))],
        compiler_params=pltpu.CompilerParams(
            collective_id=0, has_side_effects=True, vmem_limit_bytes=40 * 1024 * 1024
        ),
        cost_estimate=pl.CostEstimate(
            flops=400 * slots * owned * columns, bytes_accessed=owned * columns * 4, transcendentals=0
        ),
    )(
        jnp.stack([part.reshape(tiles) for part in (owners, offsets, next_owners, next_offsets)]),
        gradients,
    )


def split(x):
    high = x.astype(jnp.bfloat16)
    return high, (x - high.astype(jnp.float32)).astype(jnp.bfloat16)


def update(acc_ref, embedding_ref, state_ref, new_state_ref, rate_ref, table):
    half = acc_ref.shape[0]
    tiles = half // LANES
    eye = lax.broadcasted_iota(jnp.int32, (LANES, LANES), 0) == lax.broadcasted_iota(
        jnp.int32, (LANES, LANES), 1
    )
    same = jnp.where(eye, 1.0, 0.0).astype(jnp.bfloat16)
    ones = jnp.ones((2 * LANES, LANES), jnp.bfloat16)
    sides = table.shape[0] // half

    batch = min(32, tiles)

    for side in range(sides):

        @pl.loop(0, tiles // batch)
        def _(step):
            low = pl.ds(pl.multiple_of(step * batch * LANES, batch * LANES), batch * LANES)
            grad_sum = acc_ref[low, side * LANES : (side + 1) * LANES]
            square = jnp.concatenate(split(grad_sum * grad_sum), axis=1)
            sums = jnp.dot(square, ones, preferred_element_type=jnp.float32)
            means = [
                jnp.sum(
                    jnp.where(eye, sums[k * LANES : (k + 1) * LANES, :], 0.0), axis=0, keepdims=True
                )
                for k in range(batch)
            ]
            first = pl.multiple_of(side * tiles + step * batch, batch)
            rate_ref[pl.ds(first, batch), :] = jnp.concatenate(means, axis=0)

    state = state_ref[...] + rate_ref[...] * (1.0 / LANES)
    new_state_ref[...] = state
    rate_ref[...] = 0.5 * lax.rsqrt(state)

    for side in range(sides):

        @pl.loop(0, tiles // batch)
        def _(step):
            first = pl.multiple_of(side * tiles + step * batch, batch)
            rows = batch * LANES
            span = pl.ds(pl.multiple_of(first * LANES, rows), rows)
            low = pl.ds(pl.multiple_of(step * rows, rows), rows)
            parts = split(rate_ref[pl.ds(first, batch), :])
            diagonal = jnp.concatenate(
                [
                    jnp.concatenate([same * part[k : k + 1, :] for part in parts], axis=1)
                    for k in range(batch)
                ],
                axis=0,
            )
            rate = jnp.dot(diagonal, ones, preferred_element_type=jnp.float32)
            grad_sum = acc_ref[low, side * LANES : (side + 1) * LANES]
            table[span, :] = embedding_ref[span, :] - grad_sum * rate


def fetch_kernel(
    dp, rows,
    wanted_hbm, places_ref, relayed_ref, acc_ref, embedding_ref, state_ref,
    table, new_state_ref, next_ref,
    wanted_ref, picked, outgoing, incoming, relay_in, place, total, partial, summed, rate_ref,
    wanted_sem, data_send, data_recv, relay_recv, raw_sems,
):
    devices = dp * rows
    slots = outgoing.shape[0]
    capacity = slots // devices
    group = 4 if capacity == LANES else 1
    depth = group * capacity

    greet(dp, rows)
    load = pltpu.make_async_copy(wanted_hbm, wanted_ref, wanted_sem)
    load.start()
    update(acc_ref, embedding_ref, state_ref, new_state_ref, rate_ref, table)
    load.wait()

    inner = is_inner(dp)
    plane = rows * capacity
    z, r = lax.axis_index("dp"), lax.axis_index("rows")

    def span_of(i):
        return pl.ds(pl.multiple_of(i * capacity, capacity), capacity)

    def answer(dz, dr):
        i = dz * rows + dr
        return pltpu.make_async_remote_copy(
            src_ref=outgoing.at[span_of(i), :], dst_ref=incoming.at[span_of(i), :],
            send_sem=data_send.at[i], recv_sem=data_recv.at[i],
            device_id=peer(dp, rows, dz, dr), device_id_type=MESH,
        )

    def relay(dr, side):
        i = (3 - inner) * rows + dr
        k = side * rows + dr
        return pltpu.make_async_remote_copy(
            src_ref=outgoing.at[span_of(i), :], dst_ref=relay_in.at[span_of(k), :],
            send_sem=data_send.at[i], recv_sem=relay_recv.at[k],
            device_id=(z + (1 - inner) * (1 - 2 * lax.rem(z, 2)), flip(r, dr, rows)),
            device_id_type=MESH,
        )

    def send_raw():
        return pltpu.make_async_remote_copy(
            src_ref=summed, dst_ref=partial, send_sem=raw_sems.at[0], recv_sem=raw_sems.at[1],
            device_id=peer(dp, rows, 2, 0), device_id_type=MESH,
        )

    def gather(i):
        start = pl.multiple_of(i * capacity, capacity)
        for k in range(capacity):
            picked[pl.ds(k, 1), :] = table[pl.ds(wanted_ref[start + k], 1), :]
        outgoing[pl.ds(start, capacity), :] = picked[...].astype(jnp.bfloat16)

    first, second = 3 - inner, 2 + inner
    gather(first * rows)
    gathered(dp, rows)
    side = 1 - inner

    for dr in range(1, rows):
        gather(first * rows + dr)
        if dr == 1:
            pl.when(inner == 0)(lambda: relay(0, side).start())
        else:
            relay(dr - 1, side).start()
    relay(rows - 1, side).start()

    for dz in (second, 1, 0):

        @pl.loop(0, rows)
        def _(dr):
            gather(dz * rows + dr)

        for dr in range(1 if isinstance(dz, int) and dz == 0 else 0, rows):
            answer(dz, dr).start()

    lookups = total.shape[0]
    per_plane = rows // group

    def turn(source):
        for b in range(source.shape[0]):
            row = source[b : b + 1, :].astype(jnp.float32)
            place[b * LANES : (b + 1) * LANES, :] = jnp.broadcast_to(row, (LANES, LANES)).T.astype(
                jnp.int32
            )
        total[...] = jnp.zeros(total.shape, jnp.float32)

    def put(base, blocks, start):
        lane = lax.broadcasted_iota(jnp.int32, (lookups, capacity), 1)
        chosen = jnp.concatenate(
            [
                jnp.where(place[:, :capacity] == lane + (base + start + k * capacity), 1.0, 0.0)
                for k in range(group)
            ],
            axis=1,
        ).astype(jnp.bfloat16)
        total[...] += jnp.dot(
            chosen, blocks[pl.ds(start, depth), :], preferred_element_type=jnp.float32
        )

    @pl.when(inner == 1)
    def _():
        relay_in[0:capacity, :] = outgoing[2 * plane : 2 * plane + capacity, :]
        turn(relayed_ref[1])
        for half in range(2):

            @pl.loop(0, per_plane)
            def _(step):
                for k in range(group):
                    dr = step * group + k

                    def arrive():
                        relay(dr, half).wait_recv()

                    if half == 0:
                        pl.when(dr > 0)(arrive)
                    else:
                        arrive()
                start = half * plane + step * depth
                put(2 * plane, relay_in, pl.multiple_of(start, depth))

        summed[...] = total[...].astype(jnp.bfloat16)

    incoming[0:capacity, :] = outgoing[0:capacity, :]

    @pl.when(inner == 1)
    def _():
        send_raw().start()

    turn(places_ref[1])

    def take_plane(dz):
        @pl.loop(0, per_plane)
        def _(step):
            for k in range(group):
                dr = step * group + k

                def arrive():
                    answer(dz, dr).wait_recv()

                if dz == 0:
                    pl.when(dr > 0)(arrive)
                else:
                    arrive()
            put(0, incoming, pl.multiple_of(dz * plane + step * depth, depth))

    take_plane(0)
    take_plane(1)

    @pl.when(inner == 1)
    def _():
        take_plane(2)
        take_plane(3)
        next_ref[...] = total[...].astype(jnp.bfloat16)
        send_raw().wait_send()

    @pl.when(inner == 0)
    def _():
        send_raw().wait_recv()
        next_ref[...] = (total[...] + partial[...].astype(jnp.float32)).astype(jnp.bfloat16)

    @pl.loop(inner, rows)
    def _(dr):
        relay(dr, side).wait_send()

    for dz in (second, 1, 0):

        @pl.loop(1 if isinstance(dz, int) and dz == 0 else 0, rows)
        def _(dr):
            answer(dz, dr).wait_send()


def finish_kernel(*refs):
    count = len(refs) // 2
    sems = refs[-1]
    copies = []
    for source, target in zip(refs[:count], refs[count:-1]):
        pieces = 8 if source.shape[0] > 4096 else 1
        size = source.shape[0] // pieces
        for piece in range(pieces):
            span = pl.ds(piece * size, size)
            copies.append(
                pltpu.make_async_copy(
                    source.at[span, :], target.at[span, :], sems.at[len(copies)]
                )
            )
            copies[-1].start()
    for copy in copies:
        copy.wait()


def finish(*arrays):
    vmem = pl.BlockSpec(memory_space=pltpu.VMEM)
    hbm = pl.BlockSpec(memory_space=pltpu.HBM)
    return pl.pallas_call(
        finish_kernel,
        name="finish",
        out_shape=tuple(jax.ShapeDtypeStruct(array.shape, array.dtype) for array in arrays),
        in_specs=[vmem] * len(arrays),
        out_specs=(hbm,) * len(arrays),
        scratch_shapes=[pltpu.SemaphoreType.DMA((8 + len(arrays),))],
        compiler_params=pltpu.CompilerParams(vmem_limit_bytes=16 * 1024 * 1024),
    )(*arrays)


def fetch(dp, rows, wanted, places, relayed, acc, embedding, state):
    slots = wanted.shape[0]
    devices = dp * rows
    lookups = places.shape[1] * places.shape[2]
    owned, columns = embedding.shape
    tiles = (owned // LANES, LANES)
    vmem = pl.BlockSpec(memory_space=pltpu.VMEM)
    hbm = pl.BlockSpec(memory_space=pltpu.HBM)
    table, new_state, next_rows = pl.pallas_call(
        functools.partial(fetch_kernel, dp, rows),
        name="fetch",
        out_shape=(
            jax.ShapeDtypeStruct((owned, columns), jnp.float32),
            jax.ShapeDtypeStruct(tiles, jnp.float32),
            jax.ShapeDtypeStruct((lookups, columns), jnp.bfloat16),
        ),
        in_specs=[hbm] + [vmem] * 5,
        out_specs=(vmem,) * 3,
        scratch_shapes=[
            pltpu.SMEM((slots,), jnp.int32),
            pltpu.VMEM((slots // devices, columns), jnp.float32),
            pltpu.VMEM((slots, columns), jnp.bfloat16),
            pltpu.VMEM((slots, columns), jnp.bfloat16),
            pltpu.VMEM((slots // 2, columns), jnp.bfloat16),
            pltpu.VMEM((lookups, LANES), jnp.int32),
            pltpu.VMEM((lookups, columns), jnp.float32),
            pltpu.VMEM((lookups, columns), jnp.bfloat16),
            pltpu.VMEM((lookups, columns), jnp.bfloat16),
            pltpu.VMEM(tiles, jnp.float32),
            pltpu.SemaphoreType.DMA,
            pltpu.SemaphoreType.DMA((devices,)),
            pltpu.SemaphoreType.DMA((devices,)),
            pltpu.SemaphoreType.DMA((2 * rows,)),
            pltpu.SemaphoreType.DMA((2,)),
        ],
        compiler_params=pltpu.CompilerParams(
            collective_id=1, has_side_effects=True, vmem_limit_bytes=40 * 1024 * 1024
        ),
    )(wanted, places, relayed, acc, embedding, state.reshape(tiles))
    new_embedding, new_state, next_rows = finish(table, new_state, next_rows)
    return new_embedding, new_state.reshape(owned), next_rows


def on_device(owners, offsets, gradients, embedding, adagrad_state, next_owners, next_offsets):
    dp, rows = lax.axis_size("dp"), lax.axis_size("rows")
    acc, met, places, relayed = send_gradients(
        dp, rows, owners, offsets, next_owners, next_offsets, gradients, embedding.shape[0]
    )
    wanted = met[:, 0, met.shape[2] // 2 :].reshape(-1)
    new_embedding, new_state, next_rows = fetch(
        dp, rows, wanted, places, relayed, acc, embedding, adagrad_state
    )
    return (new_embedding, new_state, next_rows)


def solution(mesh):
    in_specs = (
        P(("dp", "rows"), None),
        P(("dp", "rows")),
        P(("dp", "rows"), None),
        P(("dp", "rows"), None),
        P(("dp", "rows")),
        P(("dp", "rows"), None),
        P(("dp", "rows")),
    )
    out_specs = (P(("dp", "rows"), None), P(("dp", "rows")), P(("dp", "rows"), None))
    return jax.shard_map(
        on_device, mesh=mesh, in_specs=in_specs, out_specs=out_specs, check_vma=False
    )
```

```python
import functools

import jax
import jax.numpy as jnp
from jax import lax
from jax.experimental import pallas as pl
from jax.experimental.pallas import tpu as pltpu
from jax.sharding import PartitionSpec as P

LANES = 128
SUB = 16
BASE = 256
MESH = pl.DeviceIdType.MESH


def flip(value, step, size):
    bit, result = 1, value
    while bit < size:
        own = lax.rem(lax.div(value, bit), 2)
        if isinstance(step, int):
            if step // bit % 2:
                result = result + bit * (1 - 2 * own)
        else:
            other = lax.rem(lax.div(step, bit), 2)
            result = result + bit * other * (1 - 2 * own)
        bit *= 2
    return result


def is_inner(dp):
    return lax.rem(lax.div(lax.axis_index("dp") + 1, 2), 2)


def peer(dp, rows, dz, dr):
    z, r = lax.axis_index("dp"), lax.axis_index("rows")
    return (flip(z, dz, dp), flip(r, dr, rows))


def greet(dp, rows):
    barrier = pltpu.get_barrier_semaphore()
    for i in range(1, dp * rows):
        pl.semaphore_signal(
            barrier, inc=1, device_id=peer(dp, rows, i // rows, i % rows), device_id_type=MESH
        )


def gathered(dp, rows):
    pl.semaphore_wait(pltpu.get_barrier_semaphore(), dp * rows - 1)


def selectors(names, count):
    shape = (SUB, names.shape[1])
    low = lax.broadcasted_iota(jnp.int32, shape, 0) == names % SUB
    ones = jnp.where(low, 1.0, 0.0).astype(jnp.bfloat16)
    high = jnp.broadcast_to((names // SUB).astype(jnp.float32), shape)

    def pick(start):
        shifted = (high - start).astype(jnp.bfloat16)
        zero = jnp.zeros(shape, jnp.bfloat16)
        return jnp.concatenate(
            [jnp.where(shifted == jnp.bfloat16(k), ones, zero) for k in range(count // SUB)], axis=0
        )

    return pick


def route(names, values, me, devices, capacity):
    blocks = names.shape[0]
    columns = names.shape[1]
    relative = jnp.bitwise_xor(names, me)
    index = lax.broadcasted_iota(jnp.int32, (devices, columns), 0)
    hits = [jnp.where(index == relative[b : b + 1, :], 1.0, 0.0) for b in range(blocks)]
    before = jnp.where(
        lax.broadcasted_iota(jnp.int32, (columns, columns), 0)
        < lax.broadcasted_iota(jnp.int32, (columns, columns), 1),
        1.0,
        0.0,
    ).astype(jnp.bfloat16)
    one_hot = [hit.astype(jnp.bfloat16) for hit in hits]
    ahead = jnp.dot(
        jnp.concatenate(one_hot, axis=0), before, preferred_element_type=jnp.float32
    )
    seen = jnp.zeros((devices, 1), jnp.float32)
    slots = []
    for b in range(blocks):
        within = ahead[b * devices : (b + 1) * devices, :] + seen
        slots.append(jnp.sum(hits[b] * within, axis=0, keepdims=True))
        seen = seen + jnp.sum(hits[b], axis=1, keepdims=True)
    slots = jnp.concatenate(slots, axis=0).astype(jnp.int32)
    high = (values // BASE).astype(jnp.float32)
    low = (values % BASE).astype(jnp.float32)
    place = lax.broadcasted_iota(jnp.int32, (capacity, columns), 0)
    marked = []
    for b in range(blocks):
        taken = place == slots[b : b + 1, :]
        marked.append(
            jnp.concatenate(
                [jnp.where(taken, high[b : b + 1, :], 0.0), jnp.where(taken, low[b : b + 1, :], 0.0)],
                axis=0,
            ).astype(jnp.bfloat16)
        )
    table = lax.dot_general(
        jnp.concatenate(one_hot, axis=1),
        jnp.concatenate(marked, axis=1),
        (((1,), (1,)), ((), ())),
        preferred_element_type=jnp.float32,
    )
    table = (table[:, :capacity] * BASE + table[:, capacity:]).astype(jnp.int32)
    return relative * capacity + slots, table


def send_kernel(
    dp, rows,
    index_ref, gradients_ref,
    acc_ref, met_ref, places_ref, relayed_ref,
    flat, meta_ref, outgoing, incoming, raw, relay_out,
    meta_send, meta_recv, data_send, data_recv, relay_send, raw_sems,
):
    devices = dp * rows
    slots = outgoing.shape[0]
    capacity = slots // devices
    columns = gradients_ref.shape[1]
    half = acc_ref.shape[0]
    group = 2 if capacity == LANES else 1
    depth = group * capacity

    greet(dp, rows)

    me = lax.axis_index("dp") * rows + lax.axis_index("rows")
    place, table = route(index_ref[0], index_ref[1], me, devices, capacity)
    next_place, next_table = route(index_ref[2], index_ref[3], me, devices, capacity)
    places_ref[0] = place
    places_ref[1] = next_place
    flat[...] = jnp.concatenate([table, next_table], axis=1)
    for i in range(devices):
        meta_ref[i] = flat[i : i + 1, :]

    inner = is_inner(dp)
    plane = rows * capacity
    made = min(512, plane)

    def builder(place):
        return selectors(
            jnp.concatenate([place[b : b + 1, :] for b in range(place.shape[0])], axis=1), made
        )

    def build(pick, source, target, dz, base):
        @pl.loop(0, plane // made)
        def _(step):
            first = dz * plane + step * made
            target[pl.ds(pl.multiple_of(first - base, made), made), :] = jnp.dot(
                pick(jnp.float32(first // SUB) if isinstance(first, int)
                     else (first // SUB).astype(jnp.float32)),
                source[...],
                preferred_element_type=jnp.float32,
            ).astype(jnp.bfloat16)

    def span_of(i):
        return pl.ds(pl.multiple_of(i * capacity, capacity), capacity)

    def send_meta(dz, dr):
        i = dz * rows + dr
        return pltpu.make_async_remote_copy(
            src_ref=meta_ref.at[i], dst_ref=met_ref.at[i],
            send_sem=meta_send.at[i], recv_sem=meta_recv.at[i],
            device_id=peer(dp, rows, dz, dr), device_id_type=MESH,
        )

    def send_data(dz, dr):
        i = dz * rows + dr
        return pltpu.make_async_remote_copy(
            src_ref=outgoing.at[span_of(i), :], dst_ref=incoming.at[span_of(i), :],
            send_sem=data_send.at[i], recv_sem=data_recv.at[i],
            device_id=peer(dp, rows, dz, dr), device_id_type=MESH,
        )

    def relay_data(dz, dr):
        i = dz * rows + dr
        k = i - 2 * rows
        return pltpu.make_async_remote_copy(
            src_ref=relay_out.at[span_of(k), :], dst_ref=incoming.at[span_of(i), :],
            send_sem=relay_send.at[k], recv_sem=data_recv.at[i],
            device_id=peer(dp, rows, dz - 2, dr), device_id_type=MESH,
        )

    def send_raw():
        to = peer(dp, rows, 2, 0)
        return (
            pltpu.make_async_remote_copy(
                src_ref=places_ref, dst_ref=relayed_ref,
                send_sem=raw_sems.at[0], recv_sem=raw_sems.at[1],
                device_id=to, device_id_type=MESH,
            ),
            pltpu.make_async_remote_copy(
                src_ref=gradients_ref, dst_ref=raw,
                send_sem=raw_sems.at[2], recv_sem=raw_sems.at[3],
                device_id=to, device_id_type=MESH,
            ),
        )

    pick = builder(place)
    build(pick, gradients_ref, outgoing, 1, 0)
    gathered(dp, rows)

    @pl.when(inner == 0)
    def _():
        for copy in send_raw():
            copy.start()

    for dz in (2, 1, 3, 0):
        for dr in range(0 if dz else 1, rows):
            send_meta(dz, dr).start()

    def send_plane(dz):
        for dr in range(0 if dz else 1, rows):
            send_data(dz, dr).start()

    send_plane(1)
    build(pick, gradients_ref, outgoing, 0, 0)
    send_plane(0)

    @pl.when(inner == 1)
    def _():
        for dz in (2, 3):
            build(pick, gradients_ref, outgoing, dz, 0)
            send_plane(dz)

    @pl.loop(0, half // LANES)
    def _(step):
        acc_ref[pl.ds(pl.multiple_of(step * LANES, LANES), LANES), :] = jnp.zeros(
            (LANES, acc_ref.shape[1]), jnp.float32
        )

    met_ref[0] = meta_ref[0]
    incoming[0:capacity, :] = outgoing[0:capacity, :]

    chunk = min(4096, half)

    def accumulate(tile):
        met = [met_ref[tile * group + k][:, :capacity] for k in range(group)]
        parts = []
        for k in range(group):
            side = jnp.broadcast_to((met[k] // half).astype(jnp.float32), (columns, capacity)).T
            start = pl.multiple_of((tile * group + k) * capacity, capacity)
            block = incoming[pl.ds(start, capacity), :].astype(jnp.float32)
            parts.append(
                jnp.concatenate(
                    [jnp.where(side > 0.5, 0.0, block), jnp.where(side > 0.5, block, 0.0)], axis=1
                ).astype(jnp.bfloat16)
            )
        wide = jnp.concatenate(parts, axis=0) if group > 1 else parts[0]
        names = (jnp.concatenate(met, axis=1) if group > 1 else met[0]) % half
        pick_rows = selectors(names, chunk)

        @pl.loop(0, half // chunk)
        def _(step):
            span = pl.ds(pl.multiple_of(step * chunk, chunk), chunk)
            acc_ref[span, :] += jnp.dot(
                pick_rows((step * (chunk // SUB)).astype(jnp.float32)),
                wide,
                preferred_element_type=jnp.float32,
            )

    per_plane = rows // group

    def take_plane(dz):
        @pl.loop(0, per_plane)
        def _(step):
            for k in range(group):
                dr = step * group + k

                def arrive_meta():
                    send_meta(dz, dr).wait_recv()

                def arrive():
                    send_data(dz, dr).wait_recv()

                if dz == 0:
                    pl.when(dr > 0)(arrive_meta)
                    pl.when(dr > 0)(arrive)
                elif dz == 2:
                    arrive_meta()
                    pl.when(dr + (1 - inner) > 0)(arrive)
                else:
                    arrive_meta()
                    arrive()
            accumulate(dz * per_plane + step)

    take_plane(0)

    @pl.when(inner == 1)
    def _():
        for copy in send_raw():
            copy.wait_recv()
        relay_pick = builder(relayed_ref[0])
        for dz in (3, 2):
            build(relay_pick, raw, relay_out, dz, 2 * plane)
            for dr in range(0 if dz == 3 else 1, rows):
                relay_data(dz, dr).start()
        incoming[2 * plane : 2 * plane + capacity, :] = relay_out[0:capacity, :]

    take_plane(1)
    take_plane(2)

    for dz in range(dp):

        @pl.loop(0 if dz else 1, rows)
        def _(dr):
            send_meta(dz, dr).wait_send()
            if dz < 2:
                send_data(dz, dr).wait_send()

    take_plane(3)

    @pl.when(inner == 1)
    def _():
        for dz in (2, 3):

            @pl.loop(0, rows)
            def _(dr):
                send_data(dz, dr).wait_send()

            @pl.loop(0 if dz == 3 else 1, rows)
            def _(dr):
                relay_data(dz, dr).wait_send()

    @pl.when(inner == 0)
    def _():
        for copy in send_raw():
            copy.wait_send()


def send_gradients(dp, rows, owners, offsets, next_owners, next_offsets, gradients, owned):
    devices = dp * rows
    lookups, columns = gradients.shape
    capacity = max(2, 4 * lookups // devices)
    slots = devices * capacity
    vmem = pl.BlockSpec(memory_space=pltpu.VMEM)
    tiles = (lookups // LANES, LANES)
    return pl.pallas_call(
        functools.partial(send_kernel, dp, rows),
        name="send_gradients",
        out_shape=(
            jax.ShapeDtypeStruct((owned // 2, 2 * columns), jnp.float32),
            jax.ShapeDtypeStruct((devices, 1, 2 * capacity), jnp.int32),
            jax.ShapeDtypeStruct((2,) + tiles, jnp.int32),
            jax.ShapeDtypeStruct((2,) + tiles, jnp.int32),
        ),
        in_specs=[vmem] * 2,
        out_specs=(vmem,) * 4,
        scratch_shapes=[
            pltpu.VMEM((devices, 2 * capacity), jnp.int32),
            pltpu.VMEM((devices, 1, 2 * capacity), jnp.int32),
            pltpu.VMEM((slots, columns), jnp.bfloat16),
            pltpu.VMEM((slots, columns), jnp.bfloat16),
            pltpu.VMEM((lookups, columns), jnp.bfloat16),
            pltpu.VMEM((2 * rows * capacity, columns), jnp.bfloat16),
        ]
        + [pltpu.SemaphoreType.DMA((devices,))] * 4
        + [pltpu.SemaphoreType.DMA((2 * rows,)), pltpu.SemaphoreType.DMA((4,))],
        compiler_params=pltpu.CompilerParams(
            collective_id=0, has_side_effects=True, vmem_limit_bytes=40 * 1024 * 1024
        ),
        cost_estimate=pl.CostEstimate(
            flops=400 * slots * owned * columns, bytes_accessed=owned * columns * 4, transcendentals=0
        ),
    )(
        jnp.stack([part.reshape(tiles) for part in (owners, offsets, next_owners, next_offsets)]),
        gradients,
    )


def split(x):
    high = x.astype(jnp.bfloat16)
    return high, (x - high.astype(jnp.float32)).astype(jnp.bfloat16)


def update(acc_ref, embedding_ref, state_ref, new_state_ref, rate_ref, table):
    half = acc_ref.shape[0]
    tiles = half // LANES
    eye = lax.broadcasted_iota(jnp.int32, (LANES, LANES), 0) == lax.broadcasted_iota(
        jnp.int32, (LANES, LANES), 1
    )
    same = jnp.where(eye, 1.0, 0.0).astype(jnp.bfloat16)
    ones = jnp.ones((2 * LANES, LANES), jnp.bfloat16)
    sides = table.shape[0] // half

    batch = min(32, tiles)

    for side in range(sides):

        @pl.loop(0, tiles // batch)
        def _(step):
            low = pl.ds(pl.multiple_of(step * batch * LANES, batch * LANES), batch * LANES)
            grad_sum = acc_ref[low, side * LANES : (side + 1) * LANES]
            square = jnp.concatenate(split(grad_sum * grad_sum), axis=1)
            sums = jnp.dot(square, ones, preferred_element_type=jnp.float32)
            means = [
                jnp.sum(
                    jnp.where(eye, sums[k * LANES : (k + 1) * LANES, :], 0.0), axis=0, keepdims=True
                )
                for k in range(batch)
            ]
            first = pl.multiple_of(side * tiles + step * batch, batch)
            rate_ref[pl.ds(first, batch), :] = jnp.concatenate(means, axis=0)

    state = state_ref[...] + rate_ref[...] * (1.0 / LANES)
    new_state_ref[...] = state
    rate_ref[...] = 0.5 * lax.rsqrt(state)

    for side in range(sides):

        @pl.loop(0, tiles // batch)
        def _(step):
            first = pl.multiple_of(side * tiles + step * batch, batch)
            rows = batch * LANES
            span = pl.ds(pl.multiple_of(first * LANES, rows), rows)
            low = pl.ds(pl.multiple_of(step * rows, rows), rows)
            parts = split(rate_ref[pl.ds(first, batch), :])
            diagonal = jnp.concatenate(
                [
                    jnp.concatenate([same * part[k : k + 1, :] for part in parts], axis=1)
                    for k in range(batch)
                ],
                axis=0,
            )
            rate = jnp.dot(diagonal, ones, preferred_element_type=jnp.float32)
            grad_sum = acc_ref[low, side * LANES : (side + 1) * LANES]
            table[span, :] = embedding_ref[span, :] - grad_sum * rate


def fetch_kernel(
    dp, rows,
    wanted_hbm, places_ref, relayed_ref, acc_ref, embedding_ref, state_ref,
    table, new_state_ref, next_ref,
    wanted_ref, picked, outgoing, incoming, relay_in, place, total, partial, summed, rate_ref,
    wanted_sem, data_send, data_recv, relay_recv, raw_sems,
):
    devices = dp * rows
    slots = outgoing.shape[0]
    capacity = slots // devices
    group = 4 if capacity == LANES else 1
    depth = group * capacity

    greet(dp, rows)
    load = pltpu.make_async_copy(wanted_hbm, wanted_ref, wanted_sem)
    load.start()
    update(acc_ref, embedding_ref, state_ref, new_state_ref, rate_ref, table)
    load.wait()

    inner = is_inner(dp)
    plane = rows * capacity
    z, r = lax.axis_index("dp"), lax.axis_index("rows")

    def span_of(i):
        return pl.ds(pl.multiple_of(i * capacity, capacity), capacity)

    def answer(dz, dr):
        i = dz * rows + dr
        return pltpu.make_async_remote_copy(
            src_ref=outgoing.at[span_of(i), :], dst_ref=incoming.at[span_of(i), :],
            send_sem=data_send.at[i], recv_sem=data_recv.at[i],
            device_id=peer(dp, rows, dz, dr), device_id_type=MESH,
        )

    def relay(dr, side):
        i = (3 - inner) * rows + dr
        k = side * rows + dr
        return pltpu.make_async_remote_copy(
            src_ref=outgoing.at[span_of(i), :], dst_ref=relay_in.at[span_of(k), :],
            send_sem=data_send.at[i], recv_sem=relay_recv.at[k],
            device_id=(z + (1 - inner) * (1 - 2 * lax.rem(z, 2)), flip(r, dr, rows)),
            device_id_type=MESH,
        )

    def send_raw():
        return pltpu.make_async_remote_copy(
            src_ref=summed, dst_ref=partial, send_sem=raw_sems.at[0], recv_sem=raw_sems.at[1],
            device_id=peer(dp, rows, 2, 0), device_id_type=MESH,
        )

    def gather(i):
        start = pl.multiple_of(i * capacity, capacity)
        for k in range(capacity):
            picked[pl.ds(k, 1), :] = table[pl.ds(wanted_ref[start + k], 1), :]
        outgoing[pl.ds(start, capacity), :] = picked[...].astype(jnp.bfloat16)

    first, second = 3 - inner, 2 + inner
    gather(first * rows)
    gathered(dp, rows)
    side = 1 - inner

    for dr in range(1, rows):
        gather(first * rows + dr)
        if dr == 1:
            pl.when(inner == 0)(lambda: relay(0, side).start())
        else:
            relay(dr - 1, side).start()
    relay(rows - 1, side).start()

    for dz in (second, 1, 0):

        @pl.loop(0, rows)
        def _(dr):
            gather(dz * rows + dr)

        for dr in range(1 if isinstance(dz, int) and dz == 0 else 0, rows):
            answer(dz, dr).start()

    lookups = total.shape[0]
    per_plane = rows // group

    def turn(source):
        for b in range(source.shape[0]):
            row = source[b : b + 1, :].astype(jnp.float32)
            place[b * LANES : (b + 1) * LANES, :] = jnp.broadcast_to(row, (LANES, LANES)).T.astype(
                jnp.int32
            )
        total[...] = jnp.zeros(total.shape, jnp.float32)

    def put(base, blocks, start):
        lane = lax.broadcasted_iota(jnp.int32, (lookups, capacity), 1)
        chosen = jnp.concatenate(
            [
                jnp.where(place[:, :capacity] == lane + (base + start + k * capacity), 1.0, 0.0)
                for k in range(group)
            ],
            axis=1,
        ).astype(jnp.bfloat16)
        total[...] += jnp.dot(
            chosen, blocks[pl.ds(start, depth), :], preferred_element_type=jnp.float32
        )

    @pl.when(inner == 1)
    def _():
        relay_in[0:capacity, :] = outgoing[2 * plane : 2 * plane + capacity, :]
        turn(relayed_ref[1])
        for half in range(2):

            @pl.loop(0, per_plane)
            def _(step):
                for k in range(group):
                    dr = step * group + k

                    def arrive():
                        relay(dr, half).wait_recv()

                    if half == 0:
                        pl.when(dr > 0)(arrive)
                    else:
                        arrive()
                start = half * plane + step * depth
                put(2 * plane, relay_in, pl.multiple_of(start, depth))

        summed[...] = total[...].astype(jnp.bfloat16)

    incoming[0:capacity, :] = outgoing[0:capacity, :]

    @pl.when(inner == 1)
    def _():
        send_raw().start()

    turn(places_ref[1])

    def take_plane(dz):
        @pl.loop(0, per_plane)
        def _(step):
            for k in range(group):
                dr = step * group + k

                def arrive():
                    answer(dz, dr).wait_recv()

                if dz == 0:
                    pl.when(dr > 0)(arrive)
                else:
                    arrive()
            put(0, incoming, pl.multiple_of(dz * plane + step * depth, depth))

    take_plane(0)
    take_plane(1)

    @pl.loop(inner, rows)
    def _(dr):
        relay(dr, side).wait_send()

    @pl.when(inner == 1)
    def _():
        take_plane(2)
        take_plane(3)
        next_ref[...] = total[...].astype(jnp.bfloat16)
        send_raw().wait_send()

    @pl.when(inner == 0)
    def _():
        send_raw().wait_recv()
        next_ref[...] = (total[...] + partial[...].astype(jnp.float32)).astype(jnp.bfloat16)

    for dz in (second, 1, 0):

        @pl.loop(1 if isinstance(dz, int) and dz == 0 else 0, rows)
        def _(dr):
            answer(dz, dr).wait_send()


def finish_kernel(*refs):
    count = len(refs) // 2
    sems = refs[-1]
    copies = []
    for source, target in zip(refs[:count], refs[count:-1]):
        pieces = 8 if source.shape[0] > 4096 else 1
        size = source.shape[0] // pieces
        for piece in range(pieces):
            span = pl.ds(piece * size, size)
            copies.append(
                pltpu.make_async_copy(
                    source.at[span, :], target.at[span, :], sems.at[len(copies)]
                )
            )
            copies[-1].start()
    for copy in copies:
        copy.wait()


def finish(*arrays):
    vmem = pl.BlockSpec(memory_space=pltpu.VMEM)
    hbm = pl.BlockSpec(memory_space=pltpu.HBM)
    return pl.pallas_call(
        finish_kernel,
        name="finish",
        out_shape=tuple(jax.ShapeDtypeStruct(array.shape, array.dtype) for array in arrays),
        in_specs=[vmem] * len(arrays),
        out_specs=(hbm,) * len(arrays),
        scratch_shapes=[pltpu.SemaphoreType.DMA((8 + len(arrays),))],
        compiler_params=pltpu.CompilerParams(vmem_limit_bytes=16 * 1024 * 1024),
    )(*arrays)


def fetch(dp, rows, wanted, places, relayed, acc, embedding, state):
    slots = wanted.shape[0]
    devices = dp * rows
    lookups = places.shape[1] * places.shape[2]
    owned, columns = embedding.shape
    tiles = (owned // LANES, LANES)
    vmem = pl.BlockSpec(memory_space=pltpu.VMEM)
    hbm = pl.BlockSpec(memory_space=pltpu.HBM)
    table, new_state, next_rows = pl.pallas_call(
        functools.partial(fetch_kernel, dp, rows),
        name="fetch",
        out_shape=(
            jax.ShapeDtypeStruct((owned, columns), jnp.float32),
            jax.ShapeDtypeStruct(tiles, jnp.float32),
            jax.ShapeDtypeStruct((lookups, columns), jnp.bfloat16),
        ),
        in_specs=[hbm] + [vmem] * 5,
        out_specs=(vmem,) * 3,
        scratch_shapes=[
            pltpu.SMEM((slots,), jnp.int32),
            pltpu.VMEM((slots // devices, columns), jnp.float32),
            pltpu.VMEM((slots, columns), jnp.bfloat16),
            pltpu.VMEM((slots, columns), jnp.bfloat16),
            pltpu.VMEM((slots // 2, columns), jnp.bfloat16),
            pltpu.VMEM((lookups, LANES), jnp.int32),
            pltpu.VMEM((lookups, columns), jnp.float32),
            pltpu.VMEM((lookups, columns), jnp.bfloat16),
            pltpu.VMEM((lookups, columns), jnp.bfloat16),
            pltpu.VMEM(tiles, jnp.float32),
            pltpu.SemaphoreType.DMA,
            pltpu.SemaphoreType.DMA((devices,)),
            pltpu.SemaphoreType.DMA((devices,)),
            pltpu.SemaphoreType.DMA((2 * rows,)),
            pltpu.SemaphoreType.DMA((2,)),
        ],
        compiler_params=pltpu.CompilerParams(
            collective_id=1, has_side_effects=True, vmem_limit_bytes=40 * 1024 * 1024
        ),
    )(wanted, places, relayed, acc, embedding, state.reshape(tiles))
    new_embedding, new_state, next_rows = finish(table, new_state, next_rows)
    return new_embedding, new_state.reshape(owned), next_rows


def on_device(owners, offsets, gradients, embedding, adagrad_state, next_owners, next_offsets):
    dp, rows = lax.axis_size("dp"), lax.axis_size("rows")
    acc, met, places, relayed = send_gradients(
        dp, rows, owners, offsets, next_owners, next_offsets, gradients, embedding.shape[0]
    )
    wanted = met[:, 0, met.shape[2] // 2 :].reshape(-1)
    new_embedding, new_state, next_rows = fetch(
        dp, rows, wanted, places, relayed, acc, embedding, adagrad_state
    )
    return (new_embedding, new_state, next_rows)


def solution(mesh):
    in_specs = (
        P(("dp", "rows"), None),
        P(("dp", "rows")),
        P(("dp", "rows"), None),
        P(("dp", "rows"), None),
        P(("dp", "rows")),
        P(("dp", "rows"), None),
        P(("dp", "rows")),
    )
    out_specs = (P(("dp", "rows"), None), P(("dp", "rows")), P(("dp", "rows"), None))
    return jax.shard_map(
        on_device, mesh=mesh, in_specs=in_specs, out_specs=out_specs, check_vma=False
    )
```
